32 devices in a mesh: slab: 2 (over x), grp: 16 (over z, y, core).
Axes of the slice: x: 2, y: 2, z: 4, core: 2. Of those that a mesh axis runs over, the one named last changes fastest.
Arguments:
- blocks: bfloat16 [128, 9, 256, 256], P(('slab', 'grp')), may hold values from -0.75 to 0.75
- diag_shift: float32 [32768], P(('slab', 'grp')), may hold values from 1 to 16
- offsets: int32 [128, 2], P(('slab', 'grp')), may hold values from 0 to 4
Outputs:
- factors: bfloat16 [128, 9, 256, 256], P(('slab', 'grp'))
The draws below stay inside these ranges and needn't reach their ends.
Inputs may be any that keep to these rules, and one draw needn't show every extreme that they name: offsets[i, 0] bounds from above the pattern's blocks left of the diagonal block of block row i and offsets[i, 1] those right of it; blocks that would lie outside the matrix are not in the pattern.
All inputs are finite; a program needn't handle non-finite values.
Results may differ from the reference program's by a relative error of at most 0.001.
Values may be sent and summed in bfloat16 or wider, within the bound.
A program may use at most 256 MiB of HBM per device.

```python
import math
import jax
import jax.numpy as jnp
from jax import lax

B = 256
BW = 4
RB = 4
ITERS = 2
NBR = 128
N_SLAB = 2
N_GRP = 16


def touch_ends(drawn, rng, least, high):
    place = [jax.random.randint(jax.random.fold_in(rng, axis), (), 0, length) for axis, length in enumerate(drawn.shape)]
    main_axis = drawn.shape.index(max(drawn.shape))
    next_to = place[:main_axis] + [(place[main_axis] + 1) % drawn.shape[main_axis]] + place[main_axis + 1:]
    return drawn.at[tuple(place)].set(least).at[tuple(next_to)].set(high)


def steps_of(stream_key, dims, split, low, largest):
    level, own = 1.0, jax.random.fold_in(stream_key, 6)
    for dim, blocks in split:
        steps = jnp.exp(jax.random.uniform(jax.random.fold_in(own, dim), (blocks,), jnp.float32, low / len(split), largest / len(split)))
        level = level * jnp.repeat(steps, dims[dim] // blocks).reshape([-1 if axis == dim else 1 for axis in range(len(dims))])
    return level


def bell_draw(rng, dims, width, reach, split=(), held_as=jnp.bfloat16):
    gain = steps_of(rng, dims, split, -0.22, 0.18) if split else 1.0
    drawn = jax.random.normal(rng, dims, jnp.float32) * width * gain
    return jnp.minimum(jnp.maximum(drawn, -reach), reach).astype(held_as)


def setup_inputs(seed: int = 0) -> dict:
    key_of = jax.random.split(jax.random.key(seed), 4)
    return {
        "blocks": bell_draw(key_of[0], (NBR, 2 * BW + 1, B, B), 0.05, 0.75, ((0, 32),)),
        "diag_shift": jnp.clip(jnp.exp(math.log(16.0) - 2.7725887 * jax.random.uniform(key_of[1], (NBR * B,), jnp.float32) ** steps_of(key_of[1], (NBR * B,), ((0, 32),), -0.2, 0.2)), 1.0, 16.0),
        "offsets": touch_ends(jax.random.randint(key_of[2], (NBR, 2), 0, BW + 1), jax.random.fold_in(key_of[2], 1), 0, BW).astype(jnp.int32),
    }


def band_pattern(global_rows, offsets, band_count, all_rows):
    band_reach = (band_count - 1) // 2
    relative = jnp.arange(band_count, dtype=jnp.int32) - band_reach
    lower_count = offsets[:, 0:1]
    upper_count = offsets[:, 1:2]
    target = global_rows[:, None] + relative[None, :]
    left_side = (relative < 0) & (-relative <= lower_count) & (target >= 0)
    right_side = (relative > 0) & (relative <= upper_count) & (target < all_rows)
    return (relative == 0) | left_side | right_side

def new_rows(factors_now, above_rows, scaled, present):
    band_count = factors_now.shape[1]
    band_reach = (band_count - 1) // 2
    row_count = factors_now.shape[0]
    block_size = factors_now.shape[2]
    partial_value = scaled.astype(jnp.float32)
    for offset_back in range(1, band_reach + 1):
        left_block = factors_now[:, band_reach - offset_back].astype(jnp.float32)
        upper_rows = above_rows[band_reach - offset_back:band_reach - offset_back + row_count, 1:].astype(jnp.float32)
        product = jnp.einsum('rab,rsbc->rsac', left_block, upper_rows)
        partial_value = partial_value.at[:, band_reach - offset_back + 1:2 * band_reach - offset_back + 1].add(-product)
    pieces = []
    for offset_back in range(band_reach, 0, -1):
        pivot_block = above_rows[band_reach - offset_back:band_reach - offset_back + row_count, 0].astype(jnp.float32)
        strict = jnp.triu(pivot_block, 1)
        inner_term = jnp.einsum('rab,rbc->rac', factors_now[:, band_reach - offset_back].astype(jnp.float32), strict)
        diag_values = jnp.diagonal(pivot_block, axis1=1, axis2=2)
        divisor = jnp.where(present[:, band_reach - offset_back][:, None], diag_values, 1.0)
        pieces.append((partial_value[:, band_reach - offset_back] - inner_term) / divisor[:, None, :])
    own_block = factors_now[:, band_reach].astype(jnp.float32)
    strict_lower = jnp.tril(own_block, -1)
    diag_rest = partial_value[:, band_reach] - jnp.einsum('rab,rbc->rac', strict_lower, jnp.triu(own_block, 1))
    own_diag = jnp.diagonal(own_block, axis1=1, axis2=2)
    below_mask = jnp.tril(jnp.ones((block_size, block_size), jnp.int32), -1) > 0
    pieces.append(jnp.where(below_mask[None], diag_rest / own_diag[:, None, :], diag_rest))
    upper_terms = partial_value[:, band_reach + 1:] - jnp.einsum('rab,rsbc->rsac', strict_lower, factors_now[:, band_reach + 1:].astype(jnp.float32))
    stacked = jnp.concatenate([jnp.stack(pieces, 1), upper_terms], 1)
    return jnp.where(present[:, :, None, None], stacked, 0.0).astype(jnp.bfloat16)

def reference(blocks, diag_shift, offsets):
    row_total, band_count, block_size, _ = blocks.shape
    band_reach = (band_count - 1) // 2
    shift_rows = diag_shift.reshape(row_total, block_size)
    diag_values = shift_rows + jnp.diagonal(blocks[:, band_reach].astype(jnp.float32), axis1=1, axis2=2)
    padded = jnp.pad(diag_values, ((band_reach, band_reach), (0, 0)))
    positive = padded > 0
    scales = jnp.where(positive, 1.0 / jnp.sqrt(jnp.where(positive, padded, 1.0)), 0.0)
    row_scale = scales[band_reach:band_reach + row_total]
    col_scale = jnp.stack([scales[column:column + row_total] for column in range(band_count)], 1)
    present = band_pattern(jnp.arange(row_total, dtype=jnp.int32), offsets, band_count, row_total)
    group_count = row_total // RB
    identity = jnp.eye(block_size, dtype=jnp.float32)

    def scale_group(index):
        start = (index * RB).astype(jnp.int32)
        piece = lax.dynamic_slice_in_dim(blocks, start, RB, 0).astype(jnp.float32)
        added = lax.dynamic_slice_in_dim(shift_rows, start, RB, 0)
        piece = piece.at[:, band_reach].add(identity[None] * added[:, None, :])
        rscale = lax.dynamic_slice_in_dim(row_scale, start, RB, 0)
        cscale = lax.dynamic_slice_in_dim(col_scale, start, RB, 0)
        marks = lax.dynamic_slice_in_dim(present, start, RB, 0)
        value = piece * rscale[:, None, :, None] * cscale[:, :, None, :]
        return jnp.where(marks[:, :, None, None], value, 0.0).astype(jnp.bfloat16)
    scaled = lax.map(scale_group, jnp.arange(group_count, dtype=jnp.int32)).reshape(blocks.shape)
    padded_state = jnp.concatenate([jnp.zeros((band_reach,) + blocks.shape[1:], jnp.bfloat16), scaled], 0)
    slab_rows = N_GRP * RB

    def slab_update(slab_index, padded_state):
        slab_start = (slab_index * slab_rows).astype(jnp.int32)

        def group_update(group_index):
            start = (slab_start + group_index * RB).astype(jnp.int32)
            current = lax.dynamic_slice_in_dim(padded_state, start + band_reach, RB, 0)
            above_rows = lax.dynamic_slice_in_dim(padded_state, start, RB + band_reach, 0)[:, band_reach:]
            return new_rows(current, above_rows, lax.dynamic_slice_in_dim(scaled, start, RB, 0), lax.dynamic_slice_in_dim(present, start, RB, 0))
        fresh = lax.map(group_update, jnp.arange(N_GRP, dtype=jnp.int32)).reshape((slab_rows,) + blocks.shape[1:])
        return lax.dynamic_update_slice_in_dim(padded_state, fresh, (slab_start + band_reach).astype(jnp.int32), 0)
    for sweep_index in range(ITERS):
        padded_state = lax.fori_loop(0, N_SLAB, slab_update, padded_state)
    return padded_state[band_reach:]
```

```python
import functools

import jax
import jax.numpy as jnp
from jax import lax
from jax.experimental import pallas as pl
from jax.experimental.pallas import tpu as pltpu
from jax.sharding import PartitionSpec as P

MESH = pl.DeviceIdType.MESH
F32 = jnp.float32
BF16 = jnp.bfloat16

DIAG, SHIFT, RIGHT, LEFT, AUX = 0, 4, 8, 12, 16
PIECES = 6


def kernel(
    slabs, groups, reach,
    blocks, shifts, offsets, f2,
    blk, relay, shift_own, aux_own, aux_prev, aux_next, scale, a, w1, w2, low2, h1, acc,
    load_sem, aux_load_sem, aux_send, aux_recv, send1, recv1, send2, recv2, relay_send, relay_recv,
):
    rows, band, size, _ = blk.shape
    slab, grp = lax.axis_index("slab"), lax.axis_index("grp")
    here = slab * groups + grp
    has_prev = here > 0
    has_next = here < slabs * groups - 1
    after = lax.rem(here + 1, slabs * groups)
    before = lax.rem(here + slabs * groups - 1, slabs * groups)
    nxt = (lax.div(after, groups), lax.rem(after, groups))
    prv = (lax.div(before, groups), lax.rem(before, groups))
    inner = grp < groups - 1
    edge = jnp.logical_and(grp == groups - 1, has_next)
    from_inner = grp > 0
    from_edge = jnp.logical_and(grp == 0, has_prev)

    half = size // 2
    top, low = pl.ds(0, half), pl.ds(half, half)
    cuts = ((0, top), (0, low, low), (1,), (2,), (3,), (4,))

    first, last = grp == 0, grp == groups - 1
    slab_above, slab_below = slab > 0, slab < slabs - 1
    by_last = jnp.logical_and(last, slab_above)
    by_first = jnp.logical_and(first, slab_below)
    slab_after = lax.rem(slab + 1, slabs)
    slab_before = lax.rem(slab + slabs - 1, slabs)
    ways = ((0, 1, 2, 3), (4, 5))

    def remote(src, dst, send, recv, device):
        return pltpu.make_async_remote_copy(
            src_ref=src, dst_ref=dst, send_sem=send, recv_sem=recv,
            device_id=device, device_id_type=MESH,
        )

    def start(copies):
        for copy in copies:
            copy.start()

    def wait_send(copies):
        for copy in copies:
            copy.wait_send()

    def slot(t, j, n):
        buffer = relay.at[t, j]
        if n < 2:
            return buffer.at[cuts[n]]
        return buffer.at[n - 1 if n < 4 else n - 4]

    def edge_copies(t, j, src, send):
        return [
            remote(src.at[cuts[n]], slot(t, j, n), send.at[j, n], relay_recv.at[t, j, n], device)
            for way, device in zip(ways, ((slab_after, groups - 1), (slab, 0)))
            for n in way
        ]

    def forward(t, j, way):
        goal, arrived = (w2, recv2) if t else (w1, recv1)
        device = (slab, 0) if way == 0 else (slab_after, 0)
        return [
            remote(slot(t, j, n), goal.at[j].at[cuts[n]], relay_send.at[t, j, n], arrived.at[j, n], device)
            for n in ways[way]
        ]

    def pass_on(t, j):
        for way, duty in enumerate((by_last, by_first)):
            @pl.when(duty)
            def _():
                for n, copy in zip(ways[way], forward(t, j, way)):
                    remote(
                        slot(t, j, n), slot(t, j, n), send1.at[j, n], relay_recv.at[t, j, n], nxt
                    ).wait_recv()
                    copy.start()

    def raw_copy(j):
        return remote(
            blocks.at[j, pl.ds(reach, reach + 1)], h1.at[j], send1.at[j, 0], recv1.at[j, 0], nxt
        )

    def row_copies(w, send, recv, j, pieces):
        return [
            remote(w.at[reach + j].at[cuts[n]], w.at[j].at[cuts[n]], send.at[j, n], recv.at[j, n], nxt)
            for n in pieces
        ]

    def load(j):
        others = (pl.ds(0, reach), pl.ds(reach + 1, reach))
        return [
            pltpu.make_async_copy(blocks.at[j, cut], blk.at[j, cut], load_sem.at[j, n])
            for n, cut in enumerate(others)
        ]

    def load_diagonal(j):
        return pltpu.make_async_copy(
            blocks.at[j, reach], blk.at[j, reach], load_sem.at[j, 2]
        )

    to_next = remote(aux_own, aux_prev, aux_send.at[0], aux_recv.at[0], nxt)
    to_prev = remote(
        aux_own.at[pl.ds(0, 8)], aux_next, aux_send.at[1], aux_recv.at[1], prv
    )
    shift_load = pltpu.make_async_copy(shifts, shift_own, aux_load_sem.at[0])

    shift_load.start()
    for j in range(rows):
        load_diagonal(j).start()
    for j in range(rows):
        start(load(j))

    barrier = pltpu.get_barrier_semaphore()

    def greet(flag, device):
        @pl.when(flag)
        def _():
            pl.semaphore_signal(barrier, inc=1, device_id=device, device_id_type=MESH)

    corner = jnp.logical_and(jnp.logical_or(first, last), slabs > 1)
    greet(has_prev, prv)
    greet(has_next, nxt)
    greet(corner, (slab, groups - 1 - grp))
    greet(jnp.logical_and(corner, slab_below), (slab_after, grp))
    greet(jnp.logical_and(corner, slab_above), (slab_before, grp))

    row_id = lax.broadcasted_iota(jnp.int32, (size, size), 0)
    col_id = lax.broadcasted_iota(jnp.int32, (size, size), 1)
    eye = row_id == col_id

    def scale_of(values):
        positive = values > 0
        return jnp.where(positive, 1.0 / jnp.sqrt(jnp.where(positive, values, 1.0)), 0.0)

    def as_column(row):
        return jnp.sum(jnp.where(eye, row, 0.0), axis=1, keepdims=True)

    @pl.when(jnp.logical_not(has_prev))
    def _():
        aux_prev[...] = jnp.zeros_like(aux_prev)
        for j in range(reach):
            for k in range(reach + 1):
                w1[j, k] = jnp.zeros((size, size), BF16)
                w2[j, k] = jnp.zeros((size, size), BF16)

    @pl.when(jnp.logical_not(has_next))
    def _():
        aux_next[...] = jnp.zeros_like(aux_next)

    shift_load.wait()
    for j in range(rows):
        load_diagonal(j).wait()
        diagonal = jnp.sum(
            jnp.where(eye, blk[j, reach].astype(F32), 0.0), axis=0, keepdims=True
        )
        aux_own[DIAG + j : DIAG + j + 1, :] = shift_own[j] + diagonal
        aux_own[SHIFT + j : SHIFT + j + 1, :] = shift_own[j]
        row = here * rows + j
        right = jnp.minimum(offsets[1, j], slabs * groups * rows - 1 - row)
        left = jnp.minimum(offsets[0, j], row)
        aux_own[RIGHT + j : RIGHT + j + 1, :] = jnp.full((1, size), right, jnp.int32).astype(F32)
        aux_own[LEFT + j : LEFT + j + 1, :] = jnp.full((1, size), left, jnp.int32).astype(F32)

    def count(*flags):
        return sum(flag.astype(jnp.int32) for flag in flags)

    peers = count(has_prev, has_next)
    peers = peers + count(corner) * (1 + count(slab_below, slab_above))
    pl.semaphore_wait(barrier, peers)

    @pl.when(has_next)
    def _():
        to_next.start()

    @pl.when(has_prev)
    def _():
        to_prev.start()

    @pl.when(inner)
    def _():
        for j in reversed(range(rows)):
            raw_copy(j).start()

    @pl.when(has_prev)
    def _():
        to_next.wait_recv()

    @pl.when(has_next)
    def _():
        to_prev.wait_recv()

    for j in range(rows):
        scale[j] = scale_of(aux_prev[DIAG + j : DIAG + j + 1, :])
        scale[rows + j] = scale_of(aux_own[DIAG + j : DIAG + j + 1, :])
        scale[2 * rows + j] = scale_of(aux_next[DIAG + j : DIAG + j + 1, :])

    def mask_of(table, j, k):
        place, away = (RIGHT, k - reach) if k >= reach else (LEFT, reach - k)
        return table[pl.ds(place + j, 1), :] >= away

    def scaled_block(block, table, j, k, shift, left, right):
        value = block.astype(F32)
        if k == reach:
            value = value + jnp.where(eye, shift, 0.0)
        value = value * left * right
        if k != reach:
            value = jnp.where(mask_of(table, j, k), value, 0.0)
        return value.astype(BF16)

    def scale_own(j, carry):
        for copy in load(j):
            copy.wait()
        left = as_column(scale[rows + j])
        shift = aux_own[pl.ds(SHIFT + j, 1), :]
        for k in range(band):
            value = scaled_block(blk[j, k], aux_own, j, k, shift, left, scale[j + k])
            a[j, k] = value
            if k >= reach:
                w1[reach + j, k - reach] = value
        return carry

    lax.fori_loop(0, rows, scale_own, 0)

    below = row_id > col_id

    def dot(x, y):
        return jnp.dot(x, y, preferred_element_type=F32)

    def strict_low_of(block):
        return jnp.where(below, block.astype(F32), 0.0).astype(BF16)

    def strict_up_of(block):
        return jnp.where(row_id < col_id, block.astype(F32), 0.0).astype(BF16)

    def diagonal_of(block):
        return jnp.sum(jnp.where(eye, block.astype(F32), 0.0), axis=0, keepdims=True)

    def update(j, low, w, put, before_diagonal, after_upper, wait_piece):
        def partial(k, most):
            total = a[j, k].astype(F32)
            for m in range(1, most + 1):
                s = k - reach + m
                if 1 <= s <= reach:
                    total = total - dot(low[j, reach - m], w[reach + j - m, s])
            return total

        def finish(k, value):
            if k != reach:
                value = jnp.where(mask_of(aux_own, j, k), value, 0.0)
            put(k, value.astype(BF16))

        own = w[reach + j, 0]
        strict_low = strict_low_of(own)
        for k in range(reach + 1, band):
            finish(k, partial(k, reach) - dot(strict_low, w[reach + j, k - reach]))
        before_diagonal()
        rest = partial(reach, reach) - dot(strict_low, strict_up_of(own))
        finish(reach, jnp.where(below, rest / diagonal_of(own), rest))
        after_upper()
        for k in range(1, reach):
            acc[k - 1] = partial(k, reach - 1) - dot(low[j, k], strict_up_of(w[j + k, 0]))
        for k in range(reach):
            wait_piece(k)
            pivot = w[j + k, 0]
            if k == 0:
                rest = a[j, k].astype(F32) - dot(low[j, k], strict_up_of(pivot))
            else:
                rest = acc[k - 1] - dot(low[j, 0], w[j, k])
            divisor = jnp.where(mask_of(aux_own, j, k), diagonal_of(pivot), 1.0)
            finish(k, rest / divisor)

    def nothing(*_):
        pass

    edge_pieces = range(PIECES)
    inner_pieces = range(PIECES - 1)

    def first_sweep(i, carry):
        j = rows - 1 - i

        @pl.when(from_edge)
        def _():
            for copy in row_copies(w1, send1, recv1, j, edge_pieces):
                copy.wait_recv()

        @pl.when(from_inner)
        def _():
            raw_copy(j).wait_recv()
            left = as_column(scale[j])
            shift = aux_prev[pl.ds(SHIFT + j, 1), :]
            for k in range(reach + 1):
                w1[j, k] = scaled_block(
                    h1[j, k], aux_prev, j, reach + k, shift, left, scale[j + k]
                )
            value = w1[j, reach].astype(F32) - dot(strict_low_of(w1[j, 0]), w1[j, reach])
            w2[j, reach] = jnp.where(mask_of(aux_prev, j, 2 * reach), value, 0.0).astype(BF16)

        def put(k, value):
            if k >= reach:
                w2[reach + j, k - reach] = value
            else:
                low2[j, k] = value

        update(j, a, w1, put, nothing, nothing, nothing)

        @pl.when(inner)
        def _():
            start(row_copies(w2, send2, recv2, j, inner_pieces))

        @pl.when(edge)
        def _():
            start(edge_copies(0, j, w2.at[reach + j], send1))

        return carry

    lax.fori_loop(0, rows, first_sweep, 0)

    for j in reversed(range(rows)):
        pass_on(0, j)

    def second_sweep(i, carry):
        j = rows - 1 - i
        arrivals = row_copies(w2, send2, recv2, j, edge_pieces)

        def put(k, value):
            f2[j, k] = value

        def before_diagonal():
            @pl.when(from_edge)
            def _():
                arrivals[PIECES - 1].wait_recv()

        def after_upper():
            @pl.when(edge)
            def _():
                start(edge_copies(1, j, f2.at[j, pl.ds(reach, reach + 1)], send2))

        def wait_piece(k):
            @pl.when(has_prev)
            def _():
                if k == 0:
                    arrivals[0].wait_recv()
                arrivals[k + 1].wait_recv()

        update(j, low2, w2, put, before_diagonal, after_upper, wait_piece)
        pass_on(1, j)
        return carry

    lax.fori_loop(0, rows, second_sweep, 0)

    @pl.when(has_next)
    def _():
        to_next.wait_send()

    @pl.when(has_prev)
    def _():
        to_prev.wait_send()

    @pl.when(inner)
    def _():
        for j in range(rows):
            raw_copy(j).wait_send()
            wait_send(row_copies(w2, send2, recv2, j, inner_pieces))

    @pl.when(edge)
    def _():
        for j in range(rows):
            wait_send(edge_copies(0, j, w2.at[reach + j], send1))
            wait_send(edge_copies(1, j, f2.at[j, pl.ds(reach, reach + 1)], send2))

    for way, duty in enumerate((by_last, by_first)):
        @pl.when(duty)
        def _():
            for t in range(2):
                for j in range(rows):
                    wait_send(forward(t, j, way))


def per_device(blocks, diag_shift, offsets):
    rows, band, size, _ = blocks.shape
    reach = (band - 1) // 2
    assert rows == reach == 4
    slabs, groups = lax.axis_size("slab"), lax.axis_size("grp")
    shift = diag_shift.reshape(rows, 1, size)
    block = (size, size)
    upper = (reach + 1,) + block
    dma = pltpu.SemaphoreType.DMA
    return pl.pallas_call(
        functools.partial(kernel, slabs, groups, reach),
        out_shape=pltpu.VMEM(blocks.shape, BF16),
        in_specs=[
            pl.BlockSpec(memory_space=pltpu.HBM),
            pl.BlockSpec(memory_space=pltpu.HBM),
            pl.BlockSpec(memory_space=pltpu.SMEM),
        ],
        out_specs=pl.BlockSpec(memory_space=pltpu.VMEM),
        scratch_shapes=[
            pltpu.VMEM(blocks.shape, BF16),
            pltpu.VMEM((2, rows, 3) + block, BF16),
            pltpu.VMEM((rows, 1, size), F32),
            pltpu.VMEM((AUX, size), F32),
            pltpu.VMEM((AUX, size), F32),
            pltpu.VMEM((8, size), F32),
            pltpu.VMEM((3 * rows, 1, size), F32),
            pltpu.VMEM(blocks.shape, BF16),
            pltpu.VMEM((reach + rows,) + upper, BF16),
            pltpu.VMEM((reach + rows,) + upper, BF16),
            pltpu.VMEM((rows, reach) + block, BF16),
            pltpu.VMEM((rows,) + upper, BF16),
            pltpu.VMEM((reach - 1,) + block, F32),
            dma((rows, 3)), dma((1,)), dma((2,)), dma((2,)),
            dma((rows, PIECES)), dma((rows, PIECES)), dma((rows, PIECES)), dma((rows, PIECES)),
            dma((2, rows, PIECES)), dma((2, rows, PIECES)),
        ],
        compiler_params=pltpu.CompilerParams(collective_id=0, has_side_effects=True, vmem_limit_bytes=57 << 20),
    )(blocks, shift, offsets.T)


def solution(mesh):
    return jax.shard_map(
        per_device,
        mesh=mesh,
        in_specs=(
            P(("slab", "grp"), None, None, None),
            P(("slab", "grp")),
            P(("slab", "grp"), None),
        ),
        out_specs=P(("slab", "grp"), None, None, None),
        check_vma=False,
    )
```

```python
import functools

import jax
import jax.numpy as jnp
from jax import lax
from jax.experimental import pallas as pl
from jax.experimental.pallas import tpu as pltpu
from jax.sharding import PartitionSpec as P

MESH = pl.DeviceIdType.MESH
F32 = jnp.float32
BF16 = jnp.bfloat16

DIAG, SHIFT, RIGHT, LEFT, AUX = 0, 4, 8, 12, 16
PIECES = 5
TILE = 16


def kernel(
    slabs, groups, reach,
    blocks, shifts, offsets, f2,
    blk, relay, relay_packed, packed_out, packed_in,
    shift_own, aux_own, aux_prev, aux_next, scale, a, w1, w2, low2, h1, acc,
    load_sem, aux_load_sem, aux_send, aux_recv, send1, recv1, send2, recv2, relay_send, relay_recv,
):
    rows, band, size, _ = blk.shape
    slab, grp = lax.axis_index("slab"), lax.axis_index("grp")
    here = slab * groups + grp
    has_prev = here > 0
    has_next = here < slabs * groups - 1
    after = lax.rem(here + 1, slabs * groups)
    before = lax.rem(here + slabs * groups - 1, slabs * groups)
    nxt = (lax.div(after, groups), lax.rem(after, groups))
    prv = (lax.div(before, groups), lax.rem(before, groups))
    inner = grp < groups - 1
    edge = jnp.logical_and(grp == groups - 1, has_next)
    from_inner = grp > 0
    from_edge = jnp.logical_and(grp == 0, has_prev)

    half = size // 2

    first, last = grp == 0, grp == groups - 1
    slab_above, slab_below = slab > 0, slab < slabs - 1
    by_last = jnp.logical_and(last, slab_above)
    by_first = jnp.logical_and(first, slab_below)
    slab_after = lax.rem(slab + 1, slabs)
    slab_before = lax.rem(slab + slabs - 1, slabs)
    ways = ((0, 1, 2), (3, 4))

    def remote(src, dst, send, recv, device):
        return pltpu.make_async_remote_copy(
            src_ref=src, dst_ref=dst, send_sem=send, recv_sem=recv,
            device_id=device, device_id_type=MESH,
        )

    def start(copies):
        for copy in copies:
            copy.start()

    def wait_send(copies):
        for copy in copies:
            copy.wait_send()

    def slot(t, j, n):
        return relay_packed.at[t, j] if n == 0 else relay.at[t, j, (n - 1) % 2]

    def leaving(t, j, n, src):
        return packed_out.at[t, j] if n == 0 else src.at[n]

    def landing(t, j, n):
        return packed_in.at[t, j] if n == 0 else (w2 if t else w1).at[j, n]

    def edge_copies(t, j, src, send):
        return [
            remote(leaving(t, j, n, src), slot(t, j, n), send.at[j, n], relay_recv.at[t, j, n], device)
            for way, device in zip(ways, ((slab_after, groups - 1), (slab, 0)))
            for n in way
        ]

    def forward(t, j, way):
        arrived = recv2 if t else recv1
        device = (slab, 0) if way == 0 else (slab_after, 0)
        return [
            remote(slot(t, j, n), landing(t, j, n), relay_send.at[t, j, n], arrived.at[j, n], device)
            for n in ways[way]
        ]

    def pass_on(t, j):
        for way, duty in enumerate((by_last, by_first)):
            @pl.when(duty)
            def _():
                for n, copy in zip(ways[way], forward(t, j, way)):
                    remote(
                        slot(t, j, n), slot(t, j, n), send1.at[j, n], relay_recv.at[t, j, n], nxt
                    ).wait_recv()
                    copy.start()

    def raw_copy(j):
        return remote(
            blocks.at[j, pl.ds(reach, reach + 1)], h1.at[j], send1.at[j, 0], recv1.at[j, 0], nxt
        )

    def row_copies(t, j, pieces):
        src = w2.at[reach + j]
        send, recv = (send2, recv2) if t else (send1, recv1)
        return [
            remote(leaving(0, j, n, src), landing(t, j, n), send.at[j, n], recv.at[j, n], nxt)
            for n in pieces
        ]

    def load(j):
        others = (pl.ds(0, reach), pl.ds(reach + 1, reach))
        return [
            pltpu.make_async_copy(blocks.at[j, cut], blk.at[j, cut], load_sem.at[j, n])
            for n, cut in enumerate(others)
        ]

    def load_diagonal(j):
        return pltpu.make_async_copy(
            blocks.at[j, reach], blk.at[j, reach], load_sem.at[j, 2]
        )

    to_next = remote(aux_own, aux_prev, aux_send.at[0], aux_recv.at[0], nxt)
    to_prev = remote(
        aux_own.at[pl.ds(0, 8)], aux_next, aux_send.at[1], aux_recv.at[1], prv
    )
    shift_load = pltpu.make_async_copy(shifts, shift_own, aux_load_sem.at[0])

    shift_load.start()
    for j in range(rows):
        load_diagonal(j).start()
    for j in range(rows):
        start(load(j))

    barrier = pltpu.get_barrier_semaphore()

    def greet(flag, device):
        @pl.when(flag)
        def _():
            pl.semaphore_signal(barrier, inc=1, device_id=device, device_id_type=MESH)

    corner = jnp.logical_and(jnp.logical_or(first, last), slabs > 1)
    greet(has_prev, prv)
    greet(has_next, nxt)
    greet(corner, (slab, groups - 1 - grp))
    greet(jnp.logical_and(corner, slab_below), (slab_after, grp))
    greet(jnp.logical_and(corner, slab_above), (slab_before, grp))

    row_id = lax.broadcasted_iota(jnp.int32, (size, size), 0)
    col_id = lax.broadcasted_iota(jnp.int32, (size, size), 1)
    eye = row_id == col_id

    def scale_of(values):
        positive = values > 0
        return jnp.where(positive, 1.0 / jnp.sqrt(jnp.where(positive, values, 1.0)), 0.0)

    def as_column(row):
        return jnp.sum(jnp.where(eye, row, 0.0), axis=1, keepdims=True)

    @pl.when(jnp.logical_not(has_prev))
    def _():
        aux_prev[...] = jnp.zeros_like(aux_prev)
        for j in range(reach):
            for k in range(reach + 1):
                w1[j, k] = jnp.zeros((size, size), BF16)
                w2[j, k] = jnp.zeros((size, size), BF16)

    @pl.when(jnp.logical_not(has_next))
    def _():
        aux_next[...] = jnp.zeros_like(aux_next)

    def count(*flags):
        return sum(flag.astype(jnp.int32) for flag in flags)

    peers = count(has_prev, has_next)
    peers = peers + count(corner) * (1 + count(slab_below, slab_above))
    pl.semaphore_wait(barrier, peers)

    @pl.when(inner)
    def _():
        raw_copy(rows - 1).start()

    shift_load.wait()
    for j in range(rows):
        load_diagonal(j).wait()
        diagonal = jnp.sum(
            jnp.where(eye, blk[j, reach].astype(F32), 0.0), axis=0, keepdims=True
        )
        aux_own[DIAG + j : DIAG + j + 1, :] = shift_own[j] + diagonal
        aux_own[SHIFT + j : SHIFT + j + 1, :] = shift_own[j]
        row = here * rows + j
        right = jnp.minimum(offsets[1, j], slabs * groups * rows - 1 - row)
        left = jnp.minimum(offsets[0, j], row)
        aux_own[RIGHT + j : RIGHT + j + 1, :] = jnp.full((1, size), right, jnp.int32).astype(F32)
        aux_own[LEFT + j : LEFT + j + 1, :] = jnp.full((1, size), left, jnp.int32).astype(F32)

    @pl.when(has_next)
    def _():
        to_next.start()

    @pl.when(has_prev)
    def _():
        to_prev.start()

    @pl.when(inner)
    def _():
        for j in reversed(range(rows - 1)):
            raw_copy(j).start()

    @pl.when(has_prev)
    def _():
        to_next.wait_recv()

    @pl.when(has_next)
    def _():
        to_prev.wait_recv()

    for j in range(rows):
        scale[j] = scale_of(aux_prev[DIAG + j : DIAG + j + 1, :])
        scale[rows + j] = scale_of(aux_own[DIAG + j : DIAG + j + 1, :])
        scale[2 * rows + j] = scale_of(aux_next[DIAG + j : DIAG + j + 1, :])

    def mask_of(table, j, k):
        place, away = (RIGHT, k - reach) if k >= reach else (LEFT, reach - k)
        return table[pl.ds(place + j, 1), :] >= away

    def scaled_block(block, table, j, k, shift, left, right):
        value = block.astype(F32)
        if k == reach:
            value = value + jnp.where(eye, shift, 0.0)
        value = value * left * right
        if k != reach:
            value = jnp.where(mask_of(table, j, k), value, 0.0)
        return value.astype(BF16)

    def scale_own(j, carry):
        for copy in load(j):
            copy.wait()
        left = as_column(scale[rows + j])
        shift = aux_own[pl.ds(SHIFT + j, 1), :]
        for k in range(band):
            value = scaled_block(blk[j, k], aux_own, j, k, shift, left, scale[j + k])
            a[j, k] = value
            if k >= reach:
                w1[reach + j, k - reach] = value
        return carry

    lax.fori_loop(0, rows, scale_own, 0)

    below = row_id > col_id

    def dot(x, y):
        return jnp.dot(x, y, preferred_element_type=F32)

    def strict_low_of(block):
        return jnp.where(below, block.astype(F32), 0.0).astype(BF16)

    def strict_up_of(block):
        return jnp.where(row_id < col_id, block.astype(F32), 0.0).astype(BF16)

    def diagonal_of(block):
        return jnp.sum(jnp.where(eye, block.astype(F32), 0.0), axis=0, keepdims=True)

    above = lax.broadcasted_iota(jnp.int32, (half, half), 0) < lax.broadcasted_iota(jnp.int32, (half, half), 1)

    def pack(t, j, block):
        upper, corner = block[0:half, 0:half], block[half:size, half:size]
        both = jnp.where(above, upper.astype(F32), corner.astype(F32).T)
        packed_out[t, j, 0:half, 0:half] = both.astype(BF16)
        packed_out[t, j, 0:half, half:size] = block[0:half, half:size]
        packed_out[t, j, half : half + TILE, :] = jnp.broadcast_to(
            diagonal_of(block), (TILE, size)
        ).astype(BF16)

    def unpack(t, j):
        w = w2 if t else w1
        both = packed_in[t, j, 0:half, 0:half].astype(F32)
        diagonal = packed_in[t, j, half : half + TILE, :].astype(F32)[0:1]
        on = eye[0:half, 0:half]
        for n, part in enumerate((both, both.T)):
            place = slice(n * half, (n + 1) * half)
            value = jnp.where(above, part, 0.0) + jnp.where(on, diagonal[:, place], 0.0)
            w[j, 0, place, place] = value.astype(BF16)
        w[j, 0, 0:half, half:size] = packed_in[t, j, 0:half, half:size]

    def update(j, low, w, put, before_diagonal, after_upper, wait_piece):
        def partial(k, most):
            total = a[j, k].astype(F32)
            for m in range(1, most + 1):
                s = k - reach + m
                if 1 <= s <= reach:
                    total = total - dot(low[j, reach - m], w[reach + j - m, s])
            return total

        def finish(k, value):
            if k != reach:
                value = jnp.where(mask_of(aux_own, j, k), value, 0.0)
            put(k, value.astype(BF16))

        own = w[reach + j, 0]
        strict_low = strict_low_of(own)
        for k in range(reach + 1, band):
            finish(k, partial(k, reach) - dot(strict_low, w[reach + j, k - reach]))
        before_diagonal()
        rest = partial(reach, reach) - dot(strict_low, strict_up_of(own))
        finish(reach, jnp.where(below, rest / diagonal_of(own), rest))
        after_upper()
        for k in range(1, reach):
            acc[k - 1] = partial(k, reach - 1) - dot(low[j, k], strict_up_of(w[j + k, 0]))
        for k in range(reach):
            wait_piece(k)
            pivot = w[j + k, 0]
            if k == 0:
                rest = a[j, k].astype(F32) - dot(low[j, k], strict_up_of(pivot))
            else:
                rest = acc[k - 1] - dot(low[j, 0], w[j, k])
            divisor = jnp.where(mask_of(aux_own, j, k), diagonal_of(pivot), 1.0)
            finish(k, rest / divisor)

    def nothing(*_):
        pass

    edge_pieces = range(PIECES)
    inner_pieces = range(PIECES - 1)

    def first_sweep(i, carry):
        j = rows - 1 - i

        @pl.when(from_edge)
        def _():
            for copy in row_copies(0, j, edge_pieces):
                copy.wait_recv()
            unpack(0, j)

        @pl.when(from_inner)
        def _():
            raw_copy(j).wait_recv()
            left = as_column(scale[j])
            shift = aux_prev[pl.ds(SHIFT + j, 1), :]
            for k in range(reach + 1):
                w1[j, k] = scaled_block(
                    h1[j, k], aux_prev, j, reach + k, shift, left, scale[j + k]
                )
            value = w1[j, reach].astype(F32) - dot(strict_low_of(w1[j, 0]), w1[j, reach])
            w2[j, reach] = jnp.where(mask_of(aux_prev, j, 2 * reach), value, 0.0).astype(BF16)

        def put(k, value):
            if k >= reach:
                w2[reach + j, k - reach] = value
            else:
                low2[j, k] = value

        update(j, a, w1, put, nothing, nothing, nothing)

        @pl.when(has_next)
        def _():
            pack(0, j, w2[reach + j, 0])

        @pl.when(inner)
        def _():
            start(row_copies(1, j, inner_pieces))

        @pl.when(edge)
        def _():
            start(edge_copies(0, j, w2.at[reach + j], send1))

        return carry

    lax.fori_loop(0, rows, first_sweep, 0)

    for j in reversed(range(rows)):
        pass_on(0, j)

    def second_sweep(i, carry):
        j = rows - 1 - i
        arrivals = row_copies(1, j, edge_pieces)

        def put(k, value):
            f2[j, k] = value

        def before_diagonal():
            @pl.when(from_edge)
            def _():
                arrivals[PIECES - 1].wait_recv()

        def after_upper():
            @pl.when(edge)
            def _():
                pack(1, j, f2[j, reach])
                start(edge_copies(1, j, f2.at[j, pl.ds(reach, reach + 1)], send2))

        def wait_piece(k):
            @pl.when(has_prev)
            def _():
                arrivals[k].wait_recv()
                if k == 0:
                    unpack(1, j)

        update(j, low2, w2, put, before_diagonal, after_upper, wait_piece)
        pass_on(1, j)
        return carry

    lax.fori_loop(0, rows, second_sweep, 0)

    @pl.when(has_next)
    def _():
        to_next.wait_send()

    @pl.when(has_prev)
    def _():
        to_prev.wait_send()

    @pl.when(inner)
    def _():
        for j in range(rows):
            raw_copy(j).wait_send()
            wait_send(row_copies(1, j, inner_pieces))

    @pl.when(edge)
    def _():
        for j in range(rows):
            wait_send(edge_copies(0, j, w2.at[reach + j], send1))
            wait_send(edge_copies(1, j, f2.at[j, pl.ds(reach, reach + 1)], send2))

    for way, duty in enumerate((by_last, by_first)):
        @pl.when(duty)
        def _():
            for t in range(2):
                for j in range(rows):
                    wait_send(forward(t, j, way))


def per_device(blocks, diag_shift, offsets):
    rows, band, size, _ = blocks.shape
    reach = (band - 1) // 2
    assert rows == reach == 4
    slabs, groups = lax.axis_size("slab"), lax.axis_size("grp")
    shift = diag_shift.reshape(rows, 1, size)
    block = (size, size)
    upper = (reach + 1,) + block
    dma = pltpu.SemaphoreType.DMA
    return pl.pallas_call(
        functools.partial(kernel, slabs, groups, reach),
        out_shape=pltpu.VMEM(blocks.shape, BF16),
        in_specs=[
            pl.BlockSpec(memory_space=pltpu.HBM),
            pl.BlockSpec(memory_space=pltpu.HBM),
            pl.BlockSpec(memory_space=pltpu.SMEM),
        ],
        out_specs=pl.BlockSpec(memory_space=pltpu.VMEM),
        scratch_shapes=[
            pltpu.VMEM(blocks.shape, BF16),
            pltpu.VMEM((2, rows, 2) + block, BF16),
            pltpu.VMEM((2, rows, size // 2 + TILE, size), BF16),
            pltpu.VMEM((2, rows, size // 2 + TILE, size), BF16),
            pltpu.VMEM((2, rows, size // 2 + TILE, size), BF16),
            pltpu.VMEM((rows, 1, size), F32),
            pltpu.VMEM((AUX, size), F32),
            pltpu.VMEM((AUX, size), F32),
            pltpu.VMEM((8, size), F32),
            pltpu.VMEM((3 * rows, 1, size), F32),
            pltpu.VMEM(blocks.shape, BF16),
            pltpu.VMEM((reach + rows,) + upper, BF16),
            pltpu.VMEM((reach + rows,) + upper, BF16),
            pltpu.VMEM((rows, reach) + block, BF16),
            pltpu.VMEM((rows,) + upper, BF16),
            pltpu.VMEM((reach - 1,) + block, F32),
            dma((rows, 3)), dma((1,)), dma((2,)), dma((2,)),
            dma((rows, PIECES)), dma((rows, PIECES)), dma((rows, PIECES)), dma((rows, PIECES)),
            dma((2, rows, PIECES)), dma((2, rows, PIECES)),
        ],
        compiler_params=pltpu.CompilerParams(collective_id=0, has_side_effects=True, vmem_limit_bytes=57 << 20),
    )(blocks, shift, offsets.T)


def solution(mesh):
    return jax.shard_map(
        per_device,
        mesh=mesh,
        in_specs=(
            P(("slab", "grp"), None, None, None),
            P(("slab", "grp")),
            P(("slab", "grp"), None),
        ),
        out_specs=P(("slab", "grp"), None, None, None),
        check_vma=False,
    )
```

```python
import functools

import jax
import jax.numpy as jnp
from jax import lax
from jax.experimental import pallas as pl
from jax.experimental.pallas import tpu as pltpu
from jax.sharding import PartitionSpec as P

MESH = pl.DeviceIdType.MESH
F32 = jnp.float32
BF16 = jnp.bfloat16

DIAG, SHIFT, RIGHT, LEFT, AUX = 0, 4, 8, 12, 16
TILE = 16
LOAD_FIRST, LOAD_UPPER, LOAD_LOWER, LOAD_SHIFT, LOAD_OFFSETS = range(5)


def kernel(
    slabs, groups, reach,
    blocks, shifts, offsets_in, f2,
    blk, relay, offsets, shift_own, aux_own, aux_prev, aux_next, scale, a, w1, w2, d1, d2, low2, h1, acc,
    load_sem, aux_sem, row_send, recv1, recv2, relay_recv, relay_send,
):
    rows, band, size, _ = blk.shape
    slab, grp = lax.axis_index("slab"), lax.axis_index("grp")
    here = slab * groups + grp
    has_prev = here > 0
    has_next = here < slabs * groups - 1
    after = lax.rem(here + 1, slabs * groups)
    before = lax.rem(here + slabs * groups - 1, slabs * groups)
    nxt = (lax.div(after, groups), lax.rem(after, groups))
    prv = (lax.div(before, groups), lax.rem(before, groups))
    inner = grp < groups - 1
    edge = jnp.logical_and(grp == groups - 1, has_next)
    from_inner = grp > 0
    from_edge = jnp.logical_and(grp == 0, has_prev)

    half = size // 2

    first, last = grp == 0, grp == groups - 1
    slab_above, slab_below = slab > 0, slab < slabs - 1
    by_last = jnp.logical_and(last, slab_above)
    by_first = jnp.logical_and(first, slab_below)
    slab_after = lax.rem(slab + 1, slabs)
    slab_before = lax.rem(slab + slabs - 1, slabs)
    packed = half + TILE
    tall = packed + reach * size

    def cut(n):
        return pl.ds(0, packed + size) if n == 0 else pl.ds(packed + n * size, size)

    def upper(s):
        return pl.ds(packed + (s - 1) * size, size)

    ways = ((0, 1), (2, 3))
    way_rows = (pl.ds(0, packed + 2 * size), pl.ds(0, 2 * size))

    def remote(src, dst, send, recv, device):
        return pltpu.make_async_remote_copy(
            src_ref=src, dst_ref=dst, send_sem=send, recv_sem=recv,
            device_id=device, device_id_type=MESH,
        )

    def start(copies):
        for copy in copies:
            copy.start()

    def wait_send(copies):
        for copy in copies:
            copy.wait_send()

    def only(flag, body):
        def run(_, carry):
            body()
            return carry

        lax.fori_loop(0, jnp.where(flag, 1, 0), run, 0)

    def slot(t, j, n):
        return relay.at[t, j, cut(n) if n < 2 else pl.ds((n - 2) * size, size)]

    def edge_copies(t, j):
        src, send = (w1, row_send.at[0]) if t else (w2, row_send.at[1])
        return [
            remote(src.at[reach + j, cut(n)], slot(t, j, n), send, relay_recv.at[t, j, i], device)
            for way, device in zip(ways, ((slab_after, groups - 1), (slab, 0)))
            for i, n in enumerate(way)
        ]

    def forward(t, j, way):
        device = (slab, 0) if way == 0 else (slab_after, 0)
        return [
            remote(
                slot(t, j, n), (w2 if t else w1).at[j, cut(n)], relay_send.at[0],
                recv2.at[j, n] if t else recv1.at[j, way], device,
            )
            for n in ways[way]
        ]

    def pass_on(t, j):
        for way, duty in enumerate((by_last, by_first)):
            def go():
                for i, (n, copy) in enumerate(zip(ways[way], forward(t, j, way))):
                    remote(
                        slot(t, j, n), slot(t, j, n), relay_send.at[0], relay_recv.at[t, j, i], nxt
                    ).wait_recv()
                    copy.start()

            only(duty, go)

    def raw_copy(j):
        return remote(
            blk.at[j, pl.ds(reach, reach + 1)], h1.at[j], row_send.at[0], recv1.at[j, 0], nxt
        )

    def row_copy(j, n):
        return remote(w2.at[reach + j, cut(n)], w2.at[j, cut(n)], row_send.at[1], recv2.at[j, n], nxt)

    def load(which, rows_of, cut_of):
        return pltpu.make_async_copy(
            blocks.at[rows_of, cut_of], blk.at[rows_of, cut_of], load_sem.at[which]
        )

    above_cut = pl.ds(reach, reach + 1)
    load_first = load(LOAD_FIRST, pl.ds(rows - 1, 1), above_cut)
    load_upper = load(LOAD_UPPER, pl.ds(0, rows - 1), above_cut)
    load_lower = load(LOAD_LOWER, pl.ds(0, rows), pl.ds(0, reach))
    load_shift = pltpu.make_async_copy(shifts, shift_own, load_sem.at[LOAD_SHIFT])
    load_offsets = pltpu.make_async_copy(offsets_in, offsets, load_sem.at[LOAD_OFFSETS])

    to_next = remote(aux_own, aux_prev, aux_sem.at[0], aux_sem.at[1], nxt)
    to_prev = remote(aux_own.at[pl.ds(0, 8)], aux_next, aux_sem.at[2], aux_sem.at[3], prv)

    barrier = pltpu.get_barrier_semaphore()

    def greet(flag, device):
        @pl.when(flag)
        def _():
            pl.semaphore_signal(barrier, inc=1, device_id=device, device_id_type=MESH)

    corner = jnp.logical_and(jnp.logical_or(first, last), slabs > 1)
    greet(has_prev, prv)
    greet(has_next, nxt)
    greet(corner, (slab, groups - 1 - grp))
    greet(jnp.logical_and(corner, slab_below), (slab_after, grp))
    greet(jnp.logical_and(corner, slab_above), (slab_before, grp))

    load_first.start()
    load_shift.start()
    load_offsets.start()
    load_upper.start()
    load_lower.start()

    def count(*flags):
        return sum(flag.astype(jnp.int32) for flag in flags)

    peers = count(has_prev, has_next)
    peers = peers + count(corner) * (1 + count(slab_below, slab_above))
    load_first.wait()
    pl.semaphore_wait(barrier, peers)

    @pl.when(inner)
    def _():
        raw_copy(rows - 1).start()

    row_id = lax.broadcasted_iota(jnp.int32, (size, size), 0)
    col_id = lax.broadcasted_iota(jnp.int32, (size, size), 1)
    eye = row_id == col_id

    def scale_of(values):
        positive = values > 0
        return jnp.where(positive, 1.0 / jnp.sqrt(jnp.where(positive, values, 1.0)), 0.0)

    def as_column(row):
        return jnp.sum(jnp.where(eye, row, 0.0), axis=1, keepdims=True)

    @pl.when(jnp.logical_not(has_prev))
    def _():
        aux_prev[...] = jnp.zeros_like(aux_prev)
        for w, d in ((w1, d1), (w2, d2)):
            for j in range(reach):
                w[j] = jnp.zeros((tall, size), BF16)
                d[j] = jnp.zeros((size, size), BF16)

    @pl.when(jnp.logical_not(has_next))
    def _():
        aux_next[...] = jnp.zeros_like(aux_next)

    load_shift.wait()
    load_offsets.wait()
    load_upper.wait()
    for j in range(rows):
        diagonal = jnp.sum(
            jnp.where(eye, blk[j, reach].astype(F32), 0.0), axis=0, keepdims=True
        )
        aux_own[DIAG + j : DIAG + j + 1, :] = shift_own[j] + diagonal
        aux_own[SHIFT + j : SHIFT + j + 1, :] = shift_own[j]
        row = here * rows + j
        right = jnp.minimum(offsets[1, j], slabs * groups * rows - 1 - row)
        left = jnp.minimum(offsets[0, j], row)
        aux_own[RIGHT + j : RIGHT + j + 1, :] = jnp.full((1, size), right, jnp.int32).astype(F32)
        aux_own[LEFT + j : LEFT + j + 1, :] = jnp.full((1, size), left, jnp.int32).astype(F32)

    @pl.when(has_next)
    def _():
        to_next.start()

    @pl.when(has_prev)
    def _():
        to_prev.start()

    @pl.when(inner)
    def _():
        for j in reversed(range(rows - 1)):
            raw_copy(j).start()

    @pl.when(has_prev)
    def _():
        to_next.wait_recv()

    @pl.when(has_next)
    def _():
        to_prev.wait_recv()

    for j in range(rows):
        scale[j] = scale_of(aux_prev[DIAG + j : DIAG + j + 1, :])
        scale[rows + j] = scale_of(aux_own[DIAG + j : DIAG + j + 1, :])
        scale[2 * rows + j] = scale_of(aux_next[DIAG + j : DIAG + j + 1, :])

    def mask_of(table, j, k):
        place, away = (RIGHT, k - reach) if k >= reach else (LEFT, reach - k)
        return table[pl.ds(place + j, 1), :] >= away

    def scaled_block(block, table, j, k, shift, left, right):
        value = block.astype(F32)
        if k == reach:
            value = value + jnp.where(eye, shift, 0.0)
        value = value * left * right
        if k != reach:
            value = jnp.where(mask_of(table, j, k), value, 0.0)
        return value.astype(BF16)

    def scale_own(j, carry):
        left = as_column(scale[rows + j])
        shift = aux_own[pl.ds(SHIFT + j, 1), :]
        for k in range(band):
            value = scaled_block(blk[j, k], aux_own, j, k, shift, left, scale[j + k])
            a[j, k] = value
            if k == reach:
                d1[reach + j] = value
            elif k > reach:
                w1[reach + j, upper(k - reach)] = value
        return carry

    load_lower.wait()
    lax.fori_loop(0, rows, scale_own, 0)

    below = row_id > col_id

    def dot(x, y):
        return jnp.dot(x, y, preferred_element_type=F32)

    def strict_low_of(block):
        return jnp.where(below, block.astype(F32), 0.0).astype(BF16)

    def strict_up_of(block):
        return jnp.where(row_id < col_id, block.astype(F32), 0.0).astype(BF16)

    def diagonal_of(block):
        return jnp.sum(jnp.where(eye, block.astype(F32), 0.0), axis=0, keepdims=True)

    above = lax.broadcasted_iota(jnp.int32, (half, half), 0) < lax.broadcasted_iota(jnp.int32, (half, half), 1)

    def pack(w, j, block):
        top, corner = block[0:half, 0:half], block[half:size, half:size]
        both = jnp.where(above, top.astype(F32), corner.astype(F32).T)
        w[reach + j, 0:half, 0:half] = both.astype(BF16)
        w[reach + j, 0:half, half:size] = block[0:half, half:size]
        w[reach + j, half:packed, :] = jnp.broadcast_to(diagonal_of(block), (TILE, size)).astype(BF16)

    def unpack(w, d, j):
        both = w[j, 0:half, 0:half].astype(F32)
        diagonal = w[j, half:packed, :].astype(F32)[0:1]
        on = eye[0:half, 0:half]
        for n, part in enumerate((both, both.T)):
            place = slice(n * half, (n + 1) * half)
            value = jnp.where(above, part, 0.0) + jnp.where(on, diagonal[:, place], 0.0)
            d[j, place, place] = value.astype(BF16)
        d[j, 0:half, half:size] = w[j, 0:half, half:size]

    def update(j, low, w, d, put, before_diagonal, after_upper, wait_piece):
        def partial(k, most):
            total = a[j, k].astype(F32)
            for m in range(1, most + 1):
                s = k - reach + m
                if 1 <= s <= reach:
                    total = total - dot(low[j, reach - m], w[reach + j - m, upper(s)])
            return total

        def finish(k, value):
            if k != reach:
                value = jnp.where(mask_of(aux_own, j, k), value, 0.0)
            put(k, value.astype(BF16))

        own = d[reach + j]
        strict_low = strict_low_of(own)
        for k in range(reach + 1, band):
            finish(k, partial(k, reach) - dot(strict_low, w[reach + j, upper(k - reach)]))
        before_diagonal()
        rest = partial(reach, reach) - dot(strict_low, strict_up_of(own))
        finish(reach, jnp.where(below, rest / diagonal_of(own), rest))
        after_upper()
        for k in range(1, reach):
            acc[k - 1] = partial(k, reach - 1) - dot(low[j, k], strict_up_of(d[j + k]))
        for k in range(reach):
            wait_piece(k)
            pivot = d[j + k]
            if k == 0:
                rest = a[j, k].astype(F32) - dot(low[j, k], strict_up_of(pivot))
            else:
                rest = acc[k - 1] - dot(low[j, 0], w[j, upper(k)])
            divisor = jnp.where(mask_of(aux_own, j, k), diagonal_of(pivot), 1.0)
            finish(k, rest / divisor)

    def nothing(*_):
        pass

    def first_sweep(i, carry):
        j = rows - 1 - i

        @pl.when(from_edge)
        def _():
            for way, part in enumerate(way_rows):
                remote(w1.at[j, part], w1.at[j, part], row_send.at[1], recv1.at[j, way], nxt).wait_recv()
            unpack(w1, d1, j)

        @pl.when(from_inner)
        def _():
            raw_copy(j).wait_recv()
            left = as_column(scale[j])
            shift = aux_prev[pl.ds(SHIFT + j, 1), :]
            for k in range(reach + 1):
                value = scaled_block(
                    h1[j, k], aux_prev, j, reach + k, shift, left, scale[j + k]
                )
                if k == 0:
                    d1[j] = value
                else:
                    w1[j, upper(k)] = value
            farthest = w1[j, upper(reach)]
            value = farthest.astype(F32) - dot(strict_low_of(d1[j]), farthest)
            w2[j, upper(reach)] = jnp.where(mask_of(aux_prev, j, 2 * reach), value, 0.0).astype(BF16)

        def put(k, value):
            if k == reach:
                d2[reach + j] = value
            elif k > reach:
                w2[reach + j, upper(k - reach)] = value
            else:
                low2[j, k] = value

        update(j, a, w1, d1, put, nothing, nothing, nothing)

        @pl.when(has_next)
        def _():
            pack(w2, j, d2[reach + j])

        @pl.when(inner)
        def _():
            start([row_copy(j, n) for n in range(3)])

        @pl.when(edge)
        def _():
            start(edge_copies(0, j))

        return carry

    lax.fori_loop(0, rows, first_sweep, 0)

    def pass_first(i, carry):
        pass_on(0, rows - 1 - i)
        return carry

    lax.fori_loop(0, jnp.where(jnp.logical_or(by_last, by_first), rows, 0), pass_first, 0)

    def second_sweep(i, carry):
        j = rows - 1 - i

        def put(k, value):
            f2[j, k] = value

        def before_diagonal():
            @pl.when(from_edge)
            def _():
                row_copy(j, 3).wait_recv()

        def after_upper():
            def send():
                pack(w1, j, f2[j, reach])
                for s in range(1, reach + 1):
                    w1[reach + j, upper(s)] = f2[j, reach + s]
                start(edge_copies(1, j))

            only(edge, send)
            pass_on(1, j)

        def wait_piece(k):
            if k != 1:
                @pl.when(has_prev)
                def _():
                    row_copy(j, max(k - 1, 0)).wait_recv()
                    if k == 0:
                        unpack(w2, d2, j)

        update(j, low2, w2, d2, put, before_diagonal, after_upper, wait_piece)
        return carry

    @pl.when(has_next)
    def _():
        to_next.wait_send()

    @pl.when(has_prev)
    def _():
        to_prev.wait_send()

    @pl.when(inner)
    def _():
        raw = blk.at[:, pl.ds(reach, reach + 1)]
        remote(raw, h1, row_send.at[0], recv1.at[0, 0], nxt).wait_send()

    lax.fori_loop(0, rows, second_sweep, 0)

    @pl.when(inner)
    def _():
        part = w2.at[pl.ds(reach, rows), pl.ds(0, packed + (reach - 1) * size)]
        remote(part, part, row_send.at[1], recv2.at[0, 0], nxt).wait_send()

    def sent_edge():
        for t, w in enumerate((w2, w1)):
            part = w.at[pl.ds(reach, rows)]
            remote(part, part, row_send.at[1 - t], recv2.at[0, 0], nxt).wait_send()

    only(edge, sent_edge)
    for way, duty in enumerate((by_last, by_first)):
        def passed():
            part = relay.at[:, :, way_rows[way]]
            remote(part, part, relay_send.at[0], recv2.at[0, 0], nxt).wait_send()

        only(duty, passed)


def per_device(blocks, diag_shift, offsets):
    rows, band, size, _ = blocks.shape
    reach = (band - 1) // 2
    assert rows == reach == 4
    slabs, groups = lax.axis_size("slab"), lax.axis_size("grp")
    shift = diag_shift.reshape(rows, 1, size)
    block = (size, size)
    packed = size // 2 + TILE
    tall = (reach + rows, packed + reach * size, size)
    dma = pltpu.SemaphoreType.DMA
    return pl.pallas_call(
        functools.partial(kernel, slabs, groups, reach),
        out_shape=pltpu.VMEM(blocks.shape, BF16),
        in_specs=[pl.BlockSpec(memory_space=pltpu.HBM)] * 3,
        out_specs=pl.BlockSpec(memory_space=pltpu.VMEM),
        scratch_shapes=[
            pltpu.VMEM(blocks.shape, BF16),
            pltpu.VMEM((2, rows, packed + 2 * size, size), BF16),
            pltpu.SMEM((2, rows), jnp.int32),
            pltpu.VMEM((rows, 1, size), F32),
            pltpu.VMEM((AUX, size), F32),
            pltpu.VMEM((AUX, size), F32),
            pltpu.VMEM((8, size), F32),
            pltpu.VMEM((3 * rows, 1, size), F32),
            pltpu.VMEM(blocks.shape, BF16),
            pltpu.VMEM(tall, BF16),
            pltpu.VMEM(tall, BF16),
            pltpu.VMEM((reach + rows,) + block, BF16),
            pltpu.VMEM((reach + rows,) + block, BF16),
            pltpu.VMEM((rows, reach) + block, BF16),
            pltpu.VMEM((rows, reach + 1) + block, BF16),
            pltpu.VMEM((reach - 1,) + block, F32),
            dma((5,)), dma((4,)), dma((2,)), dma((rows, 2)), dma((rows, 4)),
            dma((2, rows, 2)), dma((1,)),
        ],
        compiler_params=pltpu.CompilerParams(collective_id=0, has_side_effects=True, vmem_limit_bytes=57 << 20),
    )(blocks, shift, offsets.T)


def solution(mesh):
    return jax.shard_map(
        per_device,
        mesh=mesh,
        in_specs=(
            P(("slab", "grp"), None, None, None),
            P(("slab", "grp")),
            P(("slab", "grp"), None),
        ),
        out_specs=P(("slab", "grp"), None, None, None),
        check_vma=False,
    )
```

```python
import functools

import jax
import jax.numpy as jnp
from jax import lax
from jax.experimental import pallas as pl
from jax.experimental.pallas import tpu as pltpu
from jax.sharding import PartitionSpec as P

MESH = pl.DeviceIdType.MESH
F32 = jnp.float32
BF16 = jnp.bfloat16

DIAG, SHIFT, RIGHT, LEFT, AUX = 0, 4, 8, 12, 16
TILE = 8
LOAD_FIRST, LOAD_UPPER, LOAD_LOWER, LOAD_SHIFT, LOAD_OFFSETS = range(5)
SEND_RAW, SEND_NEXT, RELAYED, SEND_ROWS, SEND_PREV, SEND_ASIDE = range(6)
SPAN = 4


def kernel(
    slabs, groups, reach,
    blocks, shifts, offsets_in, f2,
    blk, relay, aside, offsets, shift_own, aux_own, aux_prev, aux_next, scale, a, w1, w2, d1, d2, low2, h1, acc,
    sem, aux_recv, recv1, recv2, relay_recv, aside_recv,
):
    rows, band, size, _ = blk.shape
    slab, grp = lax.axis_index("slab"), lax.axis_index("grp")
    here = slab * groups + grp
    has_prev = here > 0
    has_next = here < slabs * groups - 1
    after = lax.rem(here + 1, slabs * groups)
    before = lax.rem(here + slabs * groups - 1, slabs * groups)
    nxt = (lax.div(after, groups), lax.rem(after, groups))
    prv = (lax.div(before, groups), lax.rem(before, groups))
    inner = grp < groups - 1
    edge = jnp.logical_and(grp == groups - 1, has_next)
    from_inner = grp > 0
    from_edge = jnp.logical_and(grp == 0, has_prev)

    half = size // 2

    first, last = grp == 0, grp == groups - 1
    slab_above, slab_below = slab > 0, slab < slabs - 1
    by_last = jnp.logical_and(last, slab_above)
    by_first = jnp.logical_and(first, slab_below)
    slab_after = lax.rem(slab + 1, slabs)
    slab_before = lax.rem(slab + slabs - 1, slabs)
    packed = half + TILE
    diag = reach * size
    tall = diag + packed

    def cut(n):
        return pl.ds(2 * size, 2 * size + packed) if n == 0 else pl.ds((2 - n) * size, size)

    def upper(s):
        return pl.ds((reach - s) * size, size)

    ways = ((0,), (1, 2))
    way_rows = (pl.ds(0, packed + 2 * size), pl.ds(0, 2 * size))

    def remote(src, dst, send, recv, device):
        return pltpu.make_async_remote_copy(
            src_ref=src, dst_ref=dst, send_sem=send, recv_sem=recv,
            device_id=device, device_id_type=MESH,
        )

    def start(copies):
        for copy in copies:
            copy.start()

    def wait_send(copies):
        for copy in copies:
            copy.wait_send()

    def only(flag, body):
        def run(_, carry):
            body()
            return carry

        lax.fori_loop(0, jnp.where(flag, 1, 0), run, 0)

    def slot(t, j, n):
        return relay.at[t, j, way_rows[0] if n == 0 else pl.ds((n - 1) * size, size)]

    def edge_copies(t, j):
        src, send = (w1, sem.at[SEND_RAW]) if t else (w2, sem.at[SEND_ROWS])
        return [
            remote(src.at[reach + j, cut(n)], slot(t, j, n), send, relay_recv.at[t, j, i], device)
            for way, device in zip(ways, ((slab_after, groups - 1), (slab, 0)))
            for i, n in enumerate(way)
        ]

    def forward(t, j, way):
        device = (slab, 0) if way == 0 else (slab_after, 0)
        return [
            remote(
                slot(t, j, n), (w2 if t else w1).at[j, cut(n)], sem.at[RELAYED],
                recv2.at[j, n] if t else recv1.at[j], device,
            )
            for n in ways[way]
        ]

    def pass_on(t, j):
        for way, duty in enumerate((by_last, by_first)):
            def go():
                for i, (n, copy) in enumerate(zip(ways[way], forward(t, j, way))):
                    remote(
                        slot(t, j, n), slot(t, j, n), sem.at[RELAYED], relay_recv.at[t, j, i], nxt
                    ).wait_recv()
                    copy.start()

            only(duty, go)

    def raw_copy(j):
        return remote(
            blk.at[j, pl.ds(reach, reach + 1)], h1.at[j], sem.at[SEND_RAW], recv1.at[j], nxt
        )

    turns = aside.shape[0]
    far = jnp.logical_and(lax.rem(grp, SPAN) == SPAN - 1, inner)
    from_far = jnp.logical_and(lax.rem(grp, SPAN) == 0, grp > 0)
    inner_near = jnp.logical_and(inner, jnp.logical_not(far))

    def raw_aside():
        turn = lax.div(grp, SPAN)
        return remote(
            blk.at[0, 2 * reach], aside.at[turn], sem.at[SEND_RAW], aside_recv.at[turn], (slab, 0)
        )

    def raw_straight():
        part = pl.ds(0, reach)
        return remote(
            blk.at[0, pl.ds(reach, reach)], h1.at[0, part], sem.at[SEND_RAW], recv1.at[0], nxt
        )

    def help_on(turn):
        return remote(
            aside.at[turn], h1.at[0, reach], sem.at[SEND_ASIDE], recv1.at[0], (slab, SPAN * (turn + 1))
        )

    def row_copy(j, n):
        return remote(w2.at[reach + j, cut(n)], w2.at[j, cut(n)], sem.at[SEND_ROWS], recv2.at[j, n], nxt)

    def load(which, rows_of, cut_of):
        return pltpu.make_async_copy(
            blocks.at[rows_of, cut_of], blk.at[rows_of, cut_of], sem.at[which]
        )

    above_cut = pl.ds(reach, reach + 1)
    load_first = load(LOAD_FIRST, pl.ds(rows - 1, 1), above_cut)
    load_upper = load(LOAD_UPPER, pl.ds(0, rows - 1), above_cut)
    load_lower = load(LOAD_LOWER, pl.ds(0, rows), pl.ds(0, reach))
    load_shift = pltpu.make_async_copy(shifts, shift_own, sem.at[LOAD_SHIFT])
    load_offsets = pltpu.make_async_copy(offsets_in, offsets, sem.at[LOAD_OFFSETS])

    to_next = remote(aux_own, aux_prev, sem.at[SEND_NEXT], aux_recv.at[0], nxt)
    to_prev = remote(aux_own.at[pl.ds(0, 8)], aux_next, sem.at[SEND_PREV], aux_recv.at[1], prv)

    barrier = pltpu.get_barrier_semaphore()

    def greet(flag, device):
        @pl.when(flag)
        def _():
            pl.semaphore_signal(barrier, inc=1, device_id=device, device_id_type=MESH)

    corner = jnp.logical_and(jnp.logical_or(first, last), slabs > 1)
    greet(has_prev, prv)
    greet(has_next, nxt)
    greet(corner, (slab, groups - 1 - grp))
    greet(jnp.logical_or(far, from_far), (slab, 0))
    for turn in range(turns):
        greet(first, (slab, SPAN * turn + SPAN - 1))
    greet(jnp.logical_and(corner, slab_below), (slab_after, grp))
    greet(jnp.logical_and(corner, slab_above), (slab_before, grp))

    load_first.start()
    load_shift.start()
    load_offsets.start()
    load_upper.start()
    load_lower.start()

    def count(*flags):
        return sum(flag.astype(jnp.int32) for flag in flags)

    peers = count(has_prev, has_next)
    peers = peers + count(far) + 2 * turns * count(first)
    peers = peers + count(corner) * (1 + count(slab_below, slab_above))
    load_first.wait()
    pl.semaphore_wait(barrier, peers)

    @pl.when(inner)
    def _():
        raw_copy(rows - 1).start()

    row_id = lax.broadcasted_iota(jnp.int32, (size, size), 0)
    col_id = lax.broadcasted_iota(jnp.int32, (size, size), 1)
    eye = row_id == col_id

    def scale_of(values):
        positive = values > 0
        return jnp.where(positive, 1.0 / jnp.sqrt(jnp.where(positive, values, 1.0)), 0.0)

    def as_column(row):
        return jnp.sum(jnp.where(eye, row, 0.0), axis=1, keepdims=True)

    @pl.when(jnp.logical_not(has_prev))
    def _():
        aux_prev[...] = jnp.zeros_like(aux_prev)
        for w, d in ((w1, d1), (w2, d2)):
            for j in range(reach):
                w[j] = jnp.zeros((tall, size), BF16)
                d[j] = jnp.zeros((size, size), BF16)

    @pl.when(jnp.logical_not(has_next))
    def _():
        aux_next[...] = jnp.zeros_like(aux_next)

    load_shift.wait()
    load_offsets.wait()
    load_upper.wait()
    for j in range(rows):
        diagonal = jnp.sum(
            jnp.where(eye, blk[j, reach].astype(F32), 0.0), axis=0, keepdims=True
        )
        aux_own[DIAG + j : DIAG + j + 1, :] = shift_own[j] + diagonal
        aux_own[SHIFT + j : SHIFT + j + 1, :] = shift_own[j]
        row = here * rows + j
        right = jnp.minimum(offsets[1, j], slabs * groups * rows - 1 - row)
        left = jnp.minimum(offsets[0, j], row)
        aux_own[RIGHT + j : RIGHT + j + 1, :] = jnp.full((1, size), right, jnp.int32).astype(F32)
        aux_own[LEFT + j : LEFT + j + 1, :] = jnp.full((1, size), left, jnp.int32).astype(F32)

    @pl.when(has_next)
    def _():
        to_next.start()

    @pl.when(has_prev)
    def _():
        to_prev.start()

    @pl.when(far)
    def _():
        raw_aside().start()

    @pl.when(inner)
    def _():
        for j in reversed(range(1, rows - 1)):
            raw_copy(j).start()

    @pl.when(inner_near)
    def _():
        raw_copy(0).start()

    @pl.when(far)
    def _():
        raw_straight().start()

    @pl.when(has_prev)
    def _():
        to_next.wait_recv()

    @pl.when(has_next)
    def _():
        to_prev.wait_recv()

    for j in range(rows):
        scale[j] = scale_of(aux_prev[DIAG + j : DIAG + j + 1, :])
        scale[rows + j] = scale_of(aux_own[DIAG + j : DIAG + j + 1, :])
        scale[2 * rows + j] = scale_of(aux_next[DIAG + j : DIAG + j + 1, :])

    def mask_of(table, j, k):
        place, away = (RIGHT, k - reach) if k >= reach else (LEFT, reach - k)
        return table[pl.ds(place + j, 1), :] >= away

    def scaled_block(block, table, j, k, shift, left, right):
        value = block.astype(F32)
        if k == reach:
            value = value + jnp.where(eye, shift, 0.0)
        value = value * left * right
        if k != reach:
            value = jnp.where(mask_of(table, j, k), value, 0.0)
        return value.astype(BF16)

    def scale_own(j, carry):
        left = as_column(scale[rows + j])
        shift = aux_own[pl.ds(SHIFT + j, 1), :]
        for k in range(band):
            value = scaled_block(blk[j, k], aux_own, j, k, shift, left, scale[j + k])
            a[j, k] = value
            if k == reach:
                d1[reach + j] = value
            elif k > reach:
                w1[reach + j, upper(k - reach)] = value
        return carry

    load_lower.wait()
    lax.fori_loop(0, rows, scale_own, 0)

    def help_all():
        for turn in range(turns):
            remote(
                aside.at[turn], aside.at[turn], sem.at[SEND_ASIDE], aside_recv.at[turn], nxt
            ).wait_recv()
            help_on(turn).start()

    only(first, help_all)

    below = row_id > col_id

    def dot(x, y):
        return jnp.dot(x, y, preferred_element_type=F32)

    def strict_low_of(block):
        return jnp.where(below, block.astype(F32), 0.0).astype(BF16)

    def strict_up_of(block):
        return jnp.where(row_id < col_id, block.astype(F32), 0.0).astype(BF16)

    def diagonal_of(block):
        return jnp.sum(jnp.where(eye, block.astype(F32), 0.0), axis=0, keepdims=True)

    above = lax.broadcasted_iota(jnp.int32, (half, half), 0) < lax.broadcasted_iota(jnp.int32, (half, half), 1)

    def pack(w, j, block):
        top, corner = block[0:half, 0:half], block[half:size, half:size]
        both = jnp.where(above, top.astype(F32), corner.astype(F32).T)
        w[reach + j, diag : diag + half, 0:half] = both.astype(BF16)
        w[reach + j, diag : diag + half, half:size] = block[0:half, half:size]
        w[reach + j, diag + half : tall, :] = jnp.broadcast_to(diagonal_of(block), (TILE, size)).astype(BF16)

    def unpack(w, d, j):
        both = w[j, diag : diag + half, 0:half].astype(F32)
        diagonal = w[j, diag + half : tall, :].astype(F32)[0:1]
        on = eye[0:half, 0:half]
        for n, part in enumerate((both, both.T)):
            place = slice(n * half, (n + 1) * half)
            value = jnp.where(above, part, 0.0) + jnp.where(on, diagonal[:, place], 0.0)
            d[j, place, place] = value.astype(BF16)
        d[j, 0:half, half:size] = w[j, diag : diag + half, half:size]

    def update(j, low, w, d, put, before_diagonal, after_upper, wait_piece):
        def partial(k, most):
            total = a[j, k].astype(F32)
            for m in range(1, most + 1):
                s = k - reach + m
                if 1 <= s <= reach:
                    total = total - dot(low[j, reach - m], w[reach + j - m, upper(s)])
            return total

        def finish(k, value):
            if k != reach:
                value = jnp.where(mask_of(aux_own, j, k), value, 0.0)
            put(k, value.astype(BF16))

        own = d[reach + j]
        strict_low = strict_low_of(own)
        for k in range(reach + 1, band):
            finish(k, partial(k, reach) - dot(strict_low, w[reach + j, upper(k - reach)]))
        before_diagonal()
        rest = partial(reach, reach) - dot(strict_low, strict_up_of(own))
        finish(reach, jnp.where(below, rest / diagonal_of(own), rest))
        after_upper()
        for k in range(1, reach):
            acc[k - 1] = partial(k, reach - 1) - dot(low[j, k], strict_up_of(d[j + k]))
        for k in range(reach):
            wait_piece(k)
            pivot = d[j + k]
            if k == 0:
                rest = a[j, k].astype(F32) - dot(low[j, k], strict_up_of(pivot))
            else:
                rest = acc[k - 1] - dot(low[j, 0], w[j, upper(k)])
            divisor = jnp.where(mask_of(aux_own, j, k), diagonal_of(pivot), 1.0)
            finish(k, rest / divisor)

    def nothing(*_):
        pass

    def first_sweep(i, carry):
        j = rows - 1 - i

        @pl.when(from_edge)
        def _():
            remote(w1.at[j], w1.at[j], sem.at[SEND_ROWS], recv1.at[j], nxt).wait_recv()
            unpack(w1, d1, j)

        @pl.when(from_inner)
        def _():
            raw_copy(j).wait_recv()
            left = as_column(scale[j])
            shift = aux_prev[pl.ds(SHIFT + j, 1), :]
            for k in range(reach + 1):
                value = scaled_block(
                    h1[j, k], aux_prev, j, reach + k, shift, left, scale[j + k]
                )
                if k == 0:
                    d1[j] = value
                else:
                    w1[j, upper(k)] = value
            farthest = w1[j, upper(reach)]
            value = farthest.astype(F32) - dot(strict_low_of(d1[j]), farthest)
            w2[j, upper(reach)] = jnp.where(mask_of(aux_prev, j, 2 * reach), value, 0.0).astype(BF16)

        def put(k, value):
            if k == reach:
                d2[reach + j] = value
            elif k > reach:
                w2[reach + j, upper(k - reach)] = value
            else:
                low2[j, k] = value

        update(j, a, w1, d1, put, nothing, nothing, nothing)

        @pl.when(has_next)
        def _():
            pack(w2, j, d2[reach + j])

        @pl.when(inner)
        def _():
            start([row_copy(j, n) for n in range(2)])

        @pl.when(edge)
        def _():
            start(edge_copies(0, j))

        return carry

    lax.fori_loop(0, rows, first_sweep, 0)

    def pass_first(i, carry):
        pass_on(0, rows - 1 - i)
        return carry

    lax.fori_loop(0, jnp.where(jnp.logical_or(by_last, by_first), rows, 0), pass_first, 0)

    def second_sweep(i, carry):
        j = rows - 1 - i

        def put(k, value):
            f2[j, k] = value

        def before_diagonal():
            @pl.when(from_edge)
            def _():
                row_copy(j, 2).wait_recv()

        def after_upper():
            def send():
                pack(w1, j, f2[j, reach])
                for s in range(1, reach + 1):
                    w1[reach + j, upper(s)] = f2[j, reach + s]
                start(edge_copies(1, j))

            only(edge, send)
            pass_on(1, j)

        def wait_piece(k):
            if k in (0, reach - 1):
                @pl.when(has_prev)
                def _():
                    row_copy(j, 1 if k else 0).wait_recv()
                    if k == 0:
                        unpack(w2, d2, j)

        update(j, low2, w2, d2, put, before_diagonal, after_upper, wait_piece)
        return carry

    @pl.when(has_next)
    def _():
        to_next.wait_send()

    @pl.when(has_prev)
    def _():
        to_prev.wait_send()

    @pl.when(inner)
    def _():
        raw = blk.at[:, pl.ds(reach, reach + 1)]
        remote(raw, h1, sem.at[SEND_RAW], recv1.at[0], nxt).wait_send()

    lax.fori_loop(0, rows, second_sweep, 0)

    @pl.when(inner)
    def _():
        part = w2.at[pl.ds(reach, rows), pl.ds(size, tall - size)]
        remote(part, part, sem.at[SEND_ROWS], recv2.at[0, 0], nxt).wait_send()

    def sent_edge():
        for t, w in enumerate((w2, w1)):
            part = w.at[pl.ds(reach, rows)]
            remote(part, part, sem.at[SEND_RAW if t else SEND_ROWS], recv2.at[0, 0], nxt).wait_send()

    only(edge, sent_edge)

    def helped():
        remote(aside, aside, sem.at[SEND_ASIDE], recv2.at[0, 0], nxt).wait_send()

    only(first, helped)
    for way, duty in enumerate((by_last, by_first)):
        def passed():
            part = relay.at[:, :, way_rows[way]]
            remote(part, part, sem.at[RELAYED], recv2.at[0, 0], nxt).wait_send()

        only(duty, passed)


def per_device(blocks, diag_shift, offsets):
    rows, band, size, _ = blocks.shape
    reach = (band - 1) // 2
    assert rows == reach == 4
    slabs, groups = lax.axis_size("slab"), lax.axis_size("grp")
    shift = diag_shift.reshape(rows, 1, size)
    block = (size, size)
    packed = size // 2 + TILE
    tall = (reach + rows, packed + reach * size, size)
    dma = pltpu.SemaphoreType.DMA
    return pl.pallas_call(
        functools.partial(kernel, slabs, groups, reach),
        out_shape=pltpu.VMEM(blocks.shape, BF16),
        in_specs=[pl.BlockSpec(memory_space=pltpu.HBM)] * 3,
        out_specs=pl.BlockSpec(memory_space=pltpu.VMEM),
        scratch_shapes=[
            pltpu.VMEM(blocks.shape, BF16),
            pltpu.VMEM((2, rows, packed + 2 * size, size), BF16),
            pltpu.VMEM((groups // SPAN - 1,) + block, BF16),
            pltpu.SMEM((2, rows), jnp.int32),
            pltpu.VMEM((rows, 1, size), F32),
            pltpu.VMEM((AUX, size), F32),
            pltpu.VMEM((AUX, size), F32),
            pltpu.VMEM((8, size), F32),
            pltpu.VMEM((3 * rows, 1, size), F32),
            pltpu.VMEM(blocks.shape, BF16),
            pltpu.VMEM(tall, BF16),
            pltpu.VMEM(tall, BF16),
            pltpu.VMEM((reach + rows,) + block, BF16),
            pltpu.VMEM((reach + rows,) + block, BF16),
            pltpu.VMEM((rows, reach) + block, BF16),
            pltpu.VMEM((rows, reach + 1) + block, BF16),
            pltpu.VMEM((reach - 1,) + block, F32),
            dma((6,)), dma((2,)), dma((rows,)), dma((rows, 3)), dma((2, rows, 2)),
            dma((groups // SPAN - 1,)),
        ],
        compiler_params=pltpu.CompilerParams(collective_id=0, has_side_effects=True, vmem_limit_bytes=57 << 20),
    )(blocks, shift, offsets.T)


def solution(mesh):
    return jax.shard_map(
        per_device,
        mesh=mesh,
        in_specs=(
            P(("slab", "grp"), None, None, None),
            P(("slab", "grp")),
            P(("slab", "grp"), None),
        ),
        out_specs=P(("slab", "grp"), None, None, None),
        check_vma=False,
    )
```

```python
import functools

import jax
import jax.numpy as jnp
from jax import lax
from jax.experimental import pallas as pl
from jax.experimental.pallas import tpu as pltpu
from jax.sharding import PartitionSpec as P

MESH = pl.DeviceIdType.MESH
F32 = jnp.float32
BF16 = jnp.bfloat16

DIAG, RIGHT, LEFT, SENT, AUX = 0, 4, 8, 8, 16
TILE = 8
LOAD_FIRST, LOAD_UPPER, LOAD_LOWER, LOAD_SHIFT, LOAD_OFFSETS = range(5)
SEND_RAW, SEND_NEXT, RELAYED, SEND_ROWS, SEND_PREV, SEND_ASIDE = range(6)
SPAN = 4


def kernel(
    slabs, groups, reach,
    blocks, shifts, offsets_in, f2,
    blk, relay, aside, offsets, shift_own, aux_own, aux_prev, aux_next, scale, a, w1, w2, d1, d2, low2, h1, acc,
    sem, aux_recv, recv1, recv2, relay_recv, aside_recv,
):
    rows, band, size, _ = blk.shape
    slab, grp = lax.axis_index("slab"), lax.axis_index("grp")
    here = slab * groups + grp
    has_prev = here > 0
    has_next = here < slabs * groups - 1
    after = lax.rem(here + 1, slabs * groups)
    before = lax.rem(here + slabs * groups - 1, slabs * groups)
    nxt = (lax.div(after, groups), lax.rem(after, groups))
    prv = (lax.div(before, groups), lax.rem(before, groups))
    inner = grp < groups - 1
    edge = jnp.logical_and(grp == groups - 1, has_next)
    from_inner = grp > 0
    from_edge = jnp.logical_and(grp == 0, has_prev)

    half = size // 2

    first, last = grp == 0, grp == groups - 1
    slab_above, slab_below = slab > 0, slab < slabs - 1
    by_last = jnp.logical_and(last, slab_above)
    by_first = jnp.logical_and(first, slab_below)
    slab_after = lax.rem(slab + 1, slabs)
    slab_before = lax.rem(slab + slabs - 1, slabs)
    packed = half + TILE
    diag = reach * size
    tall = diag + packed

    whole = pl.ds(0, tall)
    most = pl.ds(size, tall - size)
    near, third = pl.ds(2 * size, 2 * size + packed), pl.ds(size, size)

    def upper(s):
        return pl.ds((reach - s) * size, size)

    ways = (near, pl.ds(0, 2 * size))

    def remote(src, dst, send, recv, device):
        return pltpu.make_async_remote_copy(
            src_ref=src, dst_ref=dst, send_sem=send, recv_sem=recv,
            device_id=device, device_id_type=MESH,
        )

    def start(copies):
        for copy in copies:
            copy.start()

    def wait_send(copies):
        for copy in copies:
            copy.wait_send()

    def only(flag, body):
        def run(_, carry):
            body()
            return carry

        lax.fori_loop(0, jnp.where(flag, 1, 0), run, 0)

    def slot(t, j, way):
        return relay.at[t, j, pl.ds(0, ways[way].size)]

    def edge_copies(t, j):
        src, send = (w1, sem.at[SEND_RAW]) if t else (w2, sem.at[SEND_ROWS])
        return [
            remote(src.at[reach + j, ways[way]], slot(t, j, way), send, relay_recv.at[t, j], device)
            for way, device in enumerate(((slab_after, groups - 1), (slab, 0)))
        ]

    def forward(t, j, way):
        return remote(
            slot(t, j, way), (w2 if t else w1).at[j, ways[way]], sem.at[RELAYED],
            (recv2 if t else recv1).at[j], (slab, 0) if way == 0 else (slab_after, 0),
        )

    def pass_on(t, j):
        for way, duty in enumerate((by_last, by_first)):
            def go():
                remote(
                    slot(t, j, way), slot(t, j, way), sem.at[RELAYED], relay_recv.at[t, j], nxt
                ).wait_recv()
                forward(t, j, way).start()

            only(duty, go)

    def raw_copy(j):
        return remote(
            blk.at[j, pl.ds(reach, reach + 1)], h1.at[j], sem.at[SEND_RAW], recv1.at[j], nxt
        )

    turns = aside.shape[0]
    far = jnp.logical_and(lax.rem(grp, SPAN) == SPAN - 1, inner)
    from_far = jnp.logical_and(lax.rem(grp, SPAN) == 0, grp > 0)
    inner_near = jnp.logical_and(inner, jnp.logical_not(far))

    def raw_aside():
        turn = lax.div(grp, SPAN)
        return remote(
            blk.at[0, 2 * reach], aside.at[turn], sem.at[SEND_RAW], aside_recv.at[0], (slab, 0)
        )

    def raw_straight():
        part = pl.ds(0, reach)
        return remote(
            blk.at[0, pl.ds(reach, reach)], h1.at[0, part], sem.at[SEND_RAW], recv1.at[0], nxt
        )

    def help_on(turn):
        return remote(
            aside.at[turn], h1.at[0, reach], sem.at[SEND_ASIDE], recv1.at[0], (slab, SPAN * (turn + 1))
        )

    def row_copy(j, part, arrived):
        return remote(w2.at[reach + j, part], w2.at[j, part], sem.at[SEND_ROWS], recv2.at[arrived], nxt)

    def load(which, rows_of, cut_of):
        return pltpu.make_async_copy(
            blocks.at[rows_of, cut_of], blk.at[rows_of, cut_of], sem.at[which]
        )

    above_cut = pl.ds(reach, reach + 1)
    load_first = load(LOAD_FIRST, pl.ds(rows - 1, 1), above_cut)
    load_upper = load(LOAD_UPPER, pl.ds(0, rows - 1), above_cut)
    load_lower = load(LOAD_LOWER, pl.ds(0, rows), pl.ds(0, reach))
    load_shift = pltpu.make_async_copy(shifts, shift_own, sem.at[LOAD_SHIFT])
    load_offsets = pltpu.make_async_copy(offsets_in, offsets, sem.at[LOAD_OFFSETS])

    to_next = remote(aux_own.at[pl.ds(0, SENT)], aux_prev, sem.at[SEND_NEXT], aux_recv.at[0], nxt)
    to_prev = remote(aux_own.at[pl.ds(0, SENT)], aux_next, sem.at[SEND_PREV], aux_recv.at[1], prv)

    barrier = pltpu.get_barrier_semaphore()

    def greet(flag, device):
        @pl.when(flag)
        def _():
            pl.semaphore_signal(barrier, inc=1, device_id=device, device_id_type=MESH)

    corner = jnp.logical_and(jnp.logical_or(first, last), slabs > 1)
    greet(has_prev, prv)
    greet(has_next, nxt)
    greet(corner, (slab, groups - 1 - grp))
    greet(jnp.logical_or(far, from_far), (slab, 0))
    for turn in range(turns):
        greet(first, (slab, SPAN * turn + SPAN - 1))
    greet(jnp.logical_and(corner, slab_below), (slab_after, grp))
    greet(jnp.logical_and(corner, slab_above), (slab_before, grp))

    load_first.start()
    load_shift.start()
    load_offsets.start()
    load_upper.start()
    load_lower.start()

    def count(*flags):
        return sum(flag.astype(jnp.int32) for flag in flags)

    peers = count(has_prev, has_next)
    peers = peers + count(far) + 2 * turns * count(first)
    peers = peers + count(corner) * (1 + count(slab_below, slab_above))
    load_first.wait()
    pl.semaphore_wait(barrier, peers)

    @pl.when(inner)
    def _():
        raw_copy(rows - 1).start()

    row_id = lax.broadcasted_iota(jnp.int32, (size, size), 0)
    col_id = lax.broadcasted_iota(jnp.int32, (size, size), 1)
    eye = row_id == col_id

    def scale_of(values):
        positive = values > 0
        return jnp.where(positive, 1.0 / jnp.sqrt(jnp.where(positive, values, 1.0)), 0.0)

    def as_column(row):
        return jnp.sum(jnp.where(eye, row, 0.0), axis=1, keepdims=True)

    @pl.when(jnp.logical_not(has_prev))
    def _():
        aux_prev[...] = jnp.zeros_like(aux_prev)
        for w, d in ((w1, d1), (w2, d2)):
            for j in range(reach):
                w[j] = jnp.zeros((tall, size), BF16)
                d[j] = jnp.zeros((size, size), BF16)

    @pl.when(jnp.logical_not(has_next))
    def _():
        aux_next[...] = jnp.zeros_like(aux_next)

    load_shift.wait()
    load_offsets.wait()
    load_upper.wait()
    for j in range(rows):
        diagonal = jnp.sum(
            jnp.where(eye, blk[j, reach].astype(F32), 0.0), axis=0, keepdims=True
        )
        aux_own[DIAG + j : DIAG + j + 1, :] = shift_own[j] + diagonal
        row = here * rows + j
        right = jnp.minimum(offsets[1, j], slabs * groups * rows - 1 - row)
        left = jnp.minimum(offsets[0, j], row)
        aux_own[RIGHT + j : RIGHT + j + 1, :] = jnp.full((1, size), right, jnp.int32).astype(F32)
        aux_own[LEFT + j : LEFT + j + 1, :] = jnp.full((1, size), left, jnp.int32).astype(F32)

    @pl.when(has_next)
    def _():
        to_next.start()

    @pl.when(has_prev)
    def _():
        to_prev.start()

    @pl.when(far)
    def _():
        raw_aside().start()

    @pl.when(inner)
    def _():
        for j in reversed(range(1, rows - 1)):
            raw_copy(j).start()

    @pl.when(inner_near)
    def _():
        raw_copy(0).start()

    @pl.when(far)
    def _():
        raw_straight().start()

    @pl.when(has_prev)
    def _():
        to_next.wait_recv()

    @pl.when(has_next)
    def _():
        to_prev.wait_recv()

    for j in range(rows):
        scale[j] = scale_of(aux_prev[DIAG + j : DIAG + j + 1, :])
        scale[rows + j] = scale_of(aux_own[DIAG + j : DIAG + j + 1, :])
        scale[2 * rows + j] = scale_of(aux_next[DIAG + j : DIAG + j + 1, :])

    def mask_of(table, j, k):
        place, away = (RIGHT, k - reach) if k >= reach else (LEFT, reach - k)
        return table[pl.ds(place + j, 1), :] >= away

    def scaled_block(block, table, j, k, left, right):
        value = block.astype(F32)
        if k == reach:
            value = jnp.where(eye, table[pl.ds(DIAG + j, 1), :], value)
        value = value * left * right
        if k != reach:
            value = jnp.where(mask_of(table, j, k), value, 0.0)
        return value.astype(BF16)

    def scale_own(j, carry):
        left = as_column(scale[rows + j])
        for k in range(band):
            value = scaled_block(blk[j, k], aux_own, j, k, left, scale[j + k])
            a[j, k] = value
            if k == reach:
                d1[reach + j] = value
            elif k > reach:
                w1[reach + j, upper(k - reach)] = value
        return carry

    load_lower.wait()
    lax.fori_loop(0, rows, scale_own, 0)

    def help_all():
        remote(aside, aside, sem.at[SEND_ASIDE], aside_recv.at[0], nxt).wait_recv()
        for turn in range(turns):
            help_on(turn).start()

    only(first, help_all)

    below = row_id > col_id

    def dot(x, y):
        return jnp.dot(x, y, preferred_element_type=F32)

    def strict_low_of(block):
        return jnp.where(below, block.astype(F32), 0.0).astype(BF16)

    def strict_up_of(block):
        return jnp.where(row_id < col_id, block.astype(F32), 0.0).astype(BF16)

    def diagonal_of(block):
        return jnp.sum(jnp.where(eye, block.astype(F32), 0.0), axis=0, keepdims=True)

    above = lax.broadcasted_iota(jnp.int32, (half, half), 0) < lax.broadcasted_iota(jnp.int32, (half, half), 1)

    def pack(w, j, block):
        top, corner = block[0:half, 0:half], block[half:size, half:size]
        both = jnp.where(above, top.astype(F32), corner.astype(F32).T)
        w[reach + j, diag : diag + half, 0:half] = both.astype(BF16)
        w[reach + j, diag : diag + half, half:size] = block[0:half, half:size]
        w[reach + j, diag + half : tall, :] = jnp.broadcast_to(diagonal_of(block), (TILE, size)).astype(BF16)

    def unpack(w, d, j):
        both = w[j, diag : diag + half, 0:half].astype(F32)
        diagonal = w[j, diag + half : tall, :].astype(F32)[0:1]
        on = eye[0:half, 0:half]
        for n, part in enumerate((both, both.T)):
            place = slice(n * half, (n + 1) * half)
            value = jnp.where(above, part, 0.0) + jnp.where(on, diagonal[:, place], 0.0)
            d[j, place, place] = value.astype(BF16)
        d[j, 0:half, half:size] = w[j, diag : diag + half, half:size]

    def update(j, low, w, d, put, before_diagonal, after_upper, wait_piece):
        def partial(k, most):
            total = a[j, k].astype(F32)
            for m in range(1, most + 1):
                s = k - reach + m
                if 1 <= s <= reach:
                    total = total - dot(low[j, reach - m], w[reach + j - m, upper(s)])
            return total

        def finish(k, value):
            if k != reach:
                value = jnp.where(mask_of(aux_own, j, k), value, 0.0)
            put(k, value.astype(BF16))

        own = d[reach + j]
        strict_low = strict_low_of(own)
        for k in range(reach + 1, band):
            finish(k, partial(k, reach) - dot(strict_low, w[reach + j, upper(k - reach)]))
        before_diagonal()
        rest = partial(reach, reach) - dot(strict_low, strict_up_of(own))
        finish(reach, jnp.where(below, rest / diagonal_of(own), rest))
        after_upper()
        for k in range(1, reach):
            acc[k - 1] = partial(k, reach - 1) - dot(low[j, k], strict_up_of(d[j + k]))
        for k in range(reach):
            wait_piece(k)
            pivot = d[j + k]
            if k == 0:
                rest = a[j, k].astype(F32) - dot(low[j, k], strict_up_of(pivot))
            else:
                rest = acc[k - 1] - dot(low[j, 0], w[j, upper(k)])
            divisor = jnp.where(mask_of(aux_own, j, k), diagonal_of(pivot), 1.0)
            finish(k, rest / divisor)

    def nothing(*_):
        pass

    def first_sweep(i, carry):
        j = rows - 1 - i

        @pl.when(from_edge)
        def _():
            remote(w1.at[j], w1.at[j], sem.at[SEND_ROWS], recv1.at[j], nxt).wait_recv()
            unpack(w1, d1, j)

        @pl.when(from_inner)
        def _():
            raw_copy(j).wait_recv()
            left = as_column(scale[j])
            for k in range(reach + 1):
                value = scaled_block(
                    h1[j, k], aux_prev, j, reach + k, left, scale[j + k]
                )
                if k == 0:
                    d1[j] = value
                else:
                    w1[j, upper(k)] = value
            farthest = w1[j, upper(reach)]
            value = farthest.astype(F32) - dot(strict_low_of(d1[j]), farthest)
            w2[j, upper(reach)] = jnp.where(mask_of(aux_prev, j, 2 * reach), value, 0.0).astype(BF16)

        def put(k, value):
            if k == reach:
                d2[reach + j] = value
            elif k > reach:
                w2[reach + j, upper(k - reach)] = value
            else:
                low2[j, k] = value

        update(j, a, w1, d1, put, nothing, nothing, nothing)

        @pl.when(has_next)
        def _():
            pack(w2, j, d2[reach + j])

        @pl.when(inner)
        def _():
            for copy, now in (
                (row_copy(j, most, j), j > 0),
                (row_copy(j, near, j), j == 0),
                (row_copy(j, third, rows), j == 0),
            ):
                pl.when(now)(copy.start)

        @pl.when(edge)
        def _():
            start(edge_copies(0, j))

        return carry

    lax.fori_loop(0, rows, first_sweep, 0)

    def pass_first(i, carry):
        pass_on(0, rows - 1 - i)
        return carry

    lax.fori_loop(0, jnp.where(jnp.logical_or(by_last, by_first), rows, 0), pass_first, 0)

    def second_sweep(i, carry):
        j = rows - 1 - i

        def put(k, value):
            f2[j, k] = value

        def before_diagonal():
            @pl.when(from_edge)
            def _():
                row_copy(j, whole, j).wait_recv()
                unpack(w2, d2, j)

        def after_upper():
            def send():
                pack(w1, j, f2[j, reach])
                for s in range(1, reach + 1):
                    w1[reach + j, upper(s)] = f2[j, reach + s]
                start(edge_copies(1, j))

            only(edge, send)
            pass_on(1, j)

        def wait_piece(k):
            if k == 0:
                @pl.when(from_inner)
                def _():
                    pl.when(j > 0)(row_copy(j, most, j).wait_recv)
                    pl.when(j == 0)(row_copy(j, near, j).wait_recv)
                    unpack(w2, d2, j)

            if k == reach - 1:
                pl.when(jnp.logical_and(from_inner, j == 0))(row_copy(j, third, rows).wait_recv)

        update(j, low2, w2, d2, put, before_diagonal, after_upper, wait_piece)
        return carry

    @pl.when(has_next)
    def _():
        to_next.wait_send()

    @pl.when(has_prev)
    def _():
        to_prev.wait_send()

    @pl.when(inner)
    def _():
        raw = blk.at[:, pl.ds(reach, reach + 1)]
        remote(raw, h1, sem.at[SEND_RAW], recv1.at[0], nxt).wait_send()

    lax.fori_loop(0, rows, second_sweep, 0)

    @pl.when(inner)
    def _():
        part = w2.at[pl.ds(reach, rows), most]
        remote(part, part, sem.at[SEND_ROWS], recv2.at[0], nxt).wait_send()

    def sent_edge():
        for t, w in enumerate((w2, w1)):
            part = w.at[pl.ds(reach, rows)]
            remote(part, part, sem.at[SEND_RAW if t else SEND_ROWS], recv2.at[0], nxt).wait_send()

    only(edge, sent_edge)

    def helped():
        remote(aside, aside, sem.at[SEND_ASIDE], recv2.at[0], nxt).wait_send()

    only(first, helped)
    for way, duty in enumerate((by_last, by_first)):
        def passed():
            part = relay.at[:, :, pl.ds(0, ways[way].size)]
            remote(part, part, sem.at[RELAYED], recv2.at[0], nxt).wait_send()

        only(duty, passed)


def per_device(blocks, diag_shift, offsets):
    rows, band, size, _ = blocks.shape
    reach = (band - 1) // 2
    assert rows == reach == 4
    slabs, groups = lax.axis_size("slab"), lax.axis_size("grp")
    shift = diag_shift.reshape(rows, 1, size)
    block = (size, size)
    packed = size // 2 + TILE
    tall = (reach + rows, packed + reach * size, size)
    dma = pltpu.SemaphoreType.DMA
    return pl.pallas_call(
        functools.partial(kernel, slabs, groups, reach),
        out_shape=pltpu.VMEM(blocks.shape, BF16),
        in_specs=[pl.BlockSpec(memory_space=pltpu.HBM)] * 3,
        out_specs=pl.BlockSpec(memory_space=pltpu.VMEM),
        scratch_shapes=[
            pltpu.VMEM(blocks.shape, BF16),
            pltpu.VMEM((2, rows, packed + 2 * size, size), BF16),
            pltpu.VMEM((groups // SPAN - 1,) + block, BF16),
            pltpu.SMEM((2, rows), jnp.int32),
            pltpu.VMEM((rows, 1, size), F32),
            pltpu.VMEM((AUX, size), F32),
            pltpu.VMEM((SENT, size), F32),
            pltpu.VMEM((SENT, size), F32),
            pltpu.VMEM((3 * rows, 1, size), F32),
            pltpu.VMEM(blocks.shape, BF16),
            pltpu.VMEM(tall, BF16),
            pltpu.VMEM(tall, BF16),
            pltpu.VMEM((reach + rows,) + block, BF16),
            pltpu.VMEM((reach + rows,) + block, BF16),
            pltpu.VMEM((rows, reach) + block, BF16),
            pltpu.VMEM((rows, reach + 1) + block, BF16),
            pltpu.VMEM((reach - 1,) + block, F32),
            dma((6,)), dma((2,)), dma((rows,)), dma((rows + 1,)), dma((2, rows)), dma((1,)),
        ],
        compiler_params=pltpu.CompilerParams(collective_id=0, has_side_effects=True, vmem_limit_bytes=57 << 20),
    )(blocks, shift, offsets.T)


def solution(mesh):
    return jax.shard_map(
        per_device,
        mesh=mesh,
        in_specs=(
            P(("slab", "grp"), None, None, None),
            P(("slab", "grp")),
            P(("slab", "grp"), None),
        ),
        out_specs=P(("slab", "grp"), None, None, None),
        check_vma=False,
    )
```

```python
import functools

import jax
import jax.numpy as jnp
from jax import lax
from jax.experimental import pallas as pl
from jax.experimental.pallas import tpu as pltpu
from jax.sharding import PartitionSpec as P

MESH = pl.DeviceIdType.MESH
F32 = jnp.float32
BF16 = jnp.bfloat16

DIAG, RIGHT, LEFT, SENT, AUX = 0, 4, 8, 8, 16
TILE = 8
LOAD_FIRST, LOAD_ROW, LOAD_LOWER, LOAD_SHIFT, LOAD_OFFSETS, LOAD_UPPER, LOAD_REST = range(7)
SEND_RAW, SEND_NEXT, RELAYED, SEND_ROWS, SEND_PREV, SEND_ASIDE, SEND_EARLY = range(7)
EARLY = 2
SPAN = 4


def kernel(
    slabs, groups, reach,
    blocks, shifts, offsets_in, f2,
    blk, relay, aside, early, offsets, shift_own, aux_own, aux_prev, aux_next, scale, a, w1, w2, d1, d2, low2, h1, acc,
    sem, aux_recv, recv1, recv2, relay_recv, aside_recv, early_recv, ready,
):
    rows, band, size, _ = blk.shape
    slab, grp = lax.axis_index("slab"), lax.axis_index("grp")
    here = slab * groups + grp
    has_prev = here > 0
    has_next = here < slabs * groups - 1
    after = lax.rem(here + 1, slabs * groups)
    before = lax.rem(here + slabs * groups - 1, slabs * groups)
    nxt = (lax.div(after, groups), lax.rem(after, groups))
    prv = (lax.div(before, groups), lax.rem(before, groups))
    inner = grp < groups - 1
    edge = jnp.logical_and(grp == groups - 1, has_next)
    from_inner = grp > 0
    from_edge = jnp.logical_and(grp == 0, has_prev)

    half = size // 2

    first, last = grp == 0, grp == groups - 1
    slab_above, slab_below = slab > 0, slab < slabs - 1
    by_last = jnp.logical_and(last, slab_above)
    by_first = jnp.logical_and(first, slab_below)
    slab_after = lax.rem(slab + 1, slabs)
    slab_before = lax.rem(slab + slabs - 1, slabs)
    packed = half + TILE
    diag = reach * size
    tall = diag + packed

    whole = pl.ds(0, tall)
    most = pl.ds(size, tall - size)
    near, third = pl.ds(2 * size, 2 * size + packed), pl.ds(size, size)

    def upper(s):
        return pl.ds((reach - s) * size, size)

    ways = (near, pl.ds(0, 2 * size))

    def remote(src, dst, send, recv, device):
        return pltpu.make_async_remote_copy(
            src_ref=src, dst_ref=dst, send_sem=send, recv_sem=recv,
            device_id=device, device_id_type=MESH,
        )

    def start(copies):
        for copy in copies:
            copy.start()

    def wait_send(copies):
        for copy in copies:
            copy.wait_send()

    def only(flag, body):
        def run(_, carry):
            body()
            return carry

        lax.fori_loop(0, jnp.where(flag, 1, 0), run, 0)

    def slot(t, j, way):
        return relay.at[t, j, pl.ds(0, ways[way].size)]

    def edge_copies(t, j):
        src, send = (w1, sem.at[SEND_RAW]) if t else (w2, sem.at[SEND_ROWS])
        return [
            remote(src.at[reach + j, ways[way]], slot(t, j, way), send, relay_recv.at[t, j], device)
            for way, device in enumerate(((slab_after, groups - 1), (slab, 0)))
        ]

    def forward(t, j, way):
        return remote(
            slot(t, j, way), (w2 if t else w1).at[j, ways[way]], sem.at[RELAYED],
            (recv2 if t else recv1).at[j], (slab, 0) if way == 0 else (slab_after, 0),
        )

    def pass_on(t, j):
        for way, duty in enumerate((by_last, by_first)):
            def go():
                remote(
                    slot(t, j, way), slot(t, j, way), sem.at[RELAYED], relay_recv.at[t, j], nxt
                ).wait_recv()
                forward(t, j, way).start()

            only(duty, go)

    def raw_copy(j):
        return remote(
            blk.at[j, pl.ds(reach, reach + 1)], h1.at[j], sem.at[SEND_RAW], recv1.at[j], nxt
        )

    turns = aside.shape[0]
    far = jnp.logical_and(lax.rem(grp, SPAN) == SPAN - 1, inner)
    from_far = jnp.logical_and(lax.rem(grp, SPAN) == 0, grp > 0)
    odd = lax.rem(grp, 2) == 1
    even = jnp.logical_not(odd)
    odd_inner, even_inner = jnp.logical_and(odd, inner), jnp.logical_and(even, inner)
    odd_near = jnp.logical_and(odd_inner, jnp.logical_not(far))
    hands_early = jnp.logical_and(odd, grp > 2)
    here_on = pl.ds(0, EARLY)
    odd_after = (slab, lax.rem(grp + 2, groups))

    def raw_early():
        return remote(
            blk.at[0, pl.ds(reach, EARLY)], early, sem.at[SEND_RAW], early_recv.at[0], odd_after
        )

    def early_on():
        return remote(early, h1.at[0, here_on], sem.at[SEND_EARLY], recv1.at[0], prv)

    def raw_aside():
        turn = lax.div(grp, SPAN)
        return remote(
            blk.at[0, 2 * reach], aside.at[turn], sem.at[SEND_RAW], aside_recv.at[0], (slab, 0)
        )

    def raw_straight(blocks_left):
        return remote(
            blk.at[0, pl.ds(reach + EARLY, blocks_left)], h1.at[0, pl.ds(EARLY, blocks_left)],
            sem.at[SEND_RAW], recv1.at[0], nxt,
        )

    def help_on(turn):
        return remote(
            aside.at[turn], h1.at[0, reach], sem.at[SEND_ASIDE], recv1.at[0], (slab, SPAN * (turn + 1))
        )

    def row_copy(j, part, arrived):
        return remote(w2.at[reach + j, part], w2.at[j, part], sem.at[SEND_ROWS], recv2.at[arrived], nxt)

    def load(which, rows_of, cut_of):
        return pltpu.make_async_copy(
            blocks.at[rows_of, cut_of], blk.at[rows_of, cut_of], sem.at[which]
        )

    above_cut = pl.ds(reach, reach + 1)
    load_first = load(LOAD_FIRST, pl.ds(0, 1), pl.ds(reach, EARLY))
    load_row = load(LOAD_ROW, pl.ds(rows - 1, 1), above_cut)
    load_upper = load(LOAD_UPPER, pl.ds(1, rows - 2), above_cut)
    load_rest = load(LOAD_REST, pl.ds(0, 1), pl.ds(reach + EARLY, reach + 1 - EARLY))
    load_lower = load(LOAD_LOWER, pl.ds(0, rows), pl.ds(0, reach))
    load_shift = pltpu.make_async_copy(shifts, shift_own, sem.at[LOAD_SHIFT])
    load_offsets = pltpu.make_async_copy(offsets_in, offsets, sem.at[LOAD_OFFSETS])

    to_next = remote(aux_own.at[pl.ds(0, SENT)], aux_prev, sem.at[SEND_NEXT], aux_recv.at[0], nxt)
    to_prev = remote(aux_own.at[pl.ds(0, SENT)], aux_next, sem.at[SEND_PREV], aux_recv.at[1], prv)

    barrier = pltpu.get_barrier_semaphore()

    def greet(flag, device):
        @pl.when(flag)
        def _():
            pl.semaphore_signal(barrier, inc=1, device_id=device, device_id_type=MESH)

    def tell(flag, n, device):
        @pl.when(flag)
        def _():
            pl.semaphore_signal(ready.at[n], inc=1, device_id=device, device_id_type=MESH)

    both = jnp.logical_and
    corner = both(jnp.logical_or(first, last), slabs > 1)
    greet(hands_early, (slab, lax.rem(grp + groups - 2, groups)))
    greet(both(odd, has_next), nxt)
    greet(odd, prv)

    load_first.start()
    load_row.start()
    load_shift.start()
    load_offsets.start()
    load_upper.start()
    load_rest.start()
    load_lower.start()

    greet(both(last, slabs > 1), (slab, 0))
    greet(both(corner, slab_below), (slab_after, grp))
    greet(both(corner, slab_above), (slab_before, grp))
    greet(jnp.logical_or(far, from_far), (slab, 0))

    def count(*flags):
        return sum(flag.astype(jnp.int32) for flag in flags)

    around = count(corner) * count(slab_below, slab_above)
    mine = count(odd_inner) + around
    theirs = count(has_prev) + 1 + count(both(first, slabs > 1)) + around + 2 * turns * count(first)
    peers = jnp.where(odd, mine, theirs)
    pl.semaphore_wait(barrier, peers)

    @pl.when(odd_inner)
    def _():
        load_first.wait()
        raw_early().start()

    tell(both(even, has_prev), 0, prv)
    tell(even, 2, nxt)
    tell(both(first, slabs > 1), 2, (slab, groups - 1))
    for turn in range(turns):
        tell(first, 1, (slab, SPAN * turn + SPAN - 1))
    pl.when(jnp.logical_not(odd_inner))(load_first.wait)
    load_row.wait()

    @pl.when(both(odd, has_next))
    def _():
        pl.semaphore_wait(ready.at[0], 1)

    @pl.when(inner)
    def _():
        raw_copy(rows - 1).start()

    row_id = lax.broadcasted_iota(jnp.int32, (size, size), 0)
    col_id = lax.broadcasted_iota(jnp.int32, (size, size), 1)
    eye = row_id == col_id

    def scale_of(values):
        positive = values > 0
        return jnp.where(positive, 1.0 / jnp.sqrt(jnp.where(positive, values, 1.0)), 0.0)

    def as_column(row):
        return jnp.sum(jnp.where(eye, row, 0.0), axis=1, keepdims=True)

    @pl.when(jnp.logical_not(has_prev))
    def _():
        aux_prev[...] = jnp.zeros_like(aux_prev)
        for w, d in ((w1, d1), (w2, d2)):
            for j in range(reach):
                w[j] = jnp.zeros((tall, size), BF16)
                d[j] = jnp.zeros((size, size), BF16)

    @pl.when(jnp.logical_not(has_next))
    def _():
        aux_next[...] = jnp.zeros_like(aux_next)

    load_shift.wait()
    load_offsets.wait()
    load_upper.wait()
    load_rest.wait()
    for j in range(rows):
        diagonal = jnp.sum(
            jnp.where(eye, blk[j, reach].astype(F32), 0.0), axis=0, keepdims=True
        )
        aux_own[DIAG + j : DIAG + j + 1, :] = shift_own[j] + diagonal
        row = here * rows + j
        right = jnp.minimum(offsets[1, j], slabs * groups * rows - 1 - row)
        left = jnp.minimum(offsets[0, j], row)
        aux_own[RIGHT + j : RIGHT + j + 1, :] = jnp.full((1, size), right, jnp.int32).astype(F32)
        aux_own[LEFT + j : LEFT + j + 1, :] = jnp.full((1, size), left, jnp.int32).astype(F32)

    @pl.when(has_next)
    def _():
        to_next.start()

    @pl.when(inner)
    def _():
        for j in reversed(range(1, rows - 1)):
            raw_copy(j).start()

    @pl.when(even_inner)
    def _():
        raw_copy(0).start()

    @pl.when(odd_near)
    def _():
        raw_straight(reach + 1 - EARLY).start()

    @pl.when(far)
    def _():
        raw_straight(reach - EARLY).start()

    @pl.when(odd)
    def _():
        pl.semaphore_wait(ready.at[2], 1 + count(both(last, slabs > 1)))

    @pl.when(has_prev)
    def _():
        to_prev.start()

    @pl.when(has_prev)
    def _():
        to_next.wait_recv()

    @pl.when(has_next)
    def _():
        to_prev.wait_recv()

    for j in range(rows):
        scale[j] = scale_of(aux_prev[DIAG + j : DIAG + j + 1, :])
        scale[rows + j] = scale_of(aux_own[DIAG + j : DIAG + j + 1, :])
        scale[2 * rows + j] = scale_of(aux_next[DIAG + j : DIAG + j + 1, :])

    def mask_of(table, j, k):
        place, away = (RIGHT, k - reach) if k >= reach else (LEFT, reach - k)
        return table[pl.ds(place + j, 1), :] >= away

    def scaled_block(block, table, j, k, left, right):
        value = block.astype(F32)
        if k == reach:
            value = jnp.where(eye, table[pl.ds(DIAG + j, 1), :], value)
        value = value * left * right
        if k != reach:
            value = jnp.where(mask_of(table, j, k), value, 0.0)
        return value.astype(BF16)

    def scale_own(j, carry):
        left = as_column(scale[rows + j])
        for k in range(band):
            value = scaled_block(blk[j, k], aux_own, j, k, left, scale[j + k])
            a[j, k] = value
            if k == reach:
                d1[reach + j] = value
            elif k > reach:
                w1[reach + j, upper(k - reach)] = value
        return carry

    load_lower.wait()
    lax.fori_loop(0, rows, scale_own, 0)

    @pl.when(far)
    def _():
        pl.semaphore_wait(ready.at[1], 1)
        raw_aside().start()

    def help_all():
        remote(aside, aside, sem.at[SEND_ASIDE], aside_recv.at[0], nxt).wait_recv()
        for turn in range(turns):
            help_on(turn).start()

    only(first, help_all)

    below = row_id > col_id

    def dot(x, y):
        return jnp.dot(x, y, preferred_element_type=F32)

    def strict_low_of(block):
        return jnp.where(below, block.astype(F32), 0.0).astype(BF16)

    def strict_up_of(block):
        return jnp.where(row_id < col_id, block.astype(F32), 0.0).astype(BF16)

    def diagonal_of(block):
        return jnp.sum(jnp.where(eye, block.astype(F32), 0.0), axis=0, keepdims=True)

    above = lax.broadcasted_iota(jnp.int32, (half, half), 0) < lax.broadcasted_iota(jnp.int32, (half, half), 1)

    def pack(w, j, block):
        top, corner = block[0:half, 0:half], block[half:size, half:size]
        both = jnp.where(above, top.astype(F32), corner.astype(F32).T)
        w[reach + j, diag : diag + half, 0:half] = both.astype(BF16)
        w[reach + j, diag : diag + half, half:size] = block[0:half, half:size]
        w[reach + j, diag + half : tall, :] = jnp.broadcast_to(diagonal_of(block), (TILE, size)).astype(BF16)

    def unpack(w, d, j):
        both = w[j, diag : diag + half, 0:half].astype(F32)
        diagonal = w[j, diag + half : tall, :].astype(F32)[0:1]
        on = eye[0:half, 0:half]
        for n, part in enumerate((both, both.T)):
            place = slice(n * half, (n + 1) * half)
            value = jnp.where(above, part, 0.0) + jnp.where(on, diagonal[:, place], 0.0)
            d[j, place, place] = value.astype(BF16)
        d[j, 0:half, half:size] = w[j, diag : diag + half, half:size]

    def update(j, low, w, d, put, before_diagonal, after_upper, wait_piece):
        def partial(k, most):
            total = a[j, k].astype(F32)
            for m in range(1, most + 1):
                s = k - reach + m
                if 1 <= s <= reach:
                    total = total - dot(low[j, reach - m], w[reach + j - m, upper(s)])
            return total

        def finish(k, value):
            if k != reach:
                value = jnp.where(mask_of(aux_own, j, k), value, 0.0)
            put(k, value.astype(BF16))

        own = d[reach + j]
        strict_low = strict_low_of(own)
        for k in range(reach + 1, band):
            finish(k, partial(k, reach) - dot(strict_low, w[reach + j, upper(k - reach)]))
        before_diagonal()
        rest = partial(reach, reach) - dot(strict_low, strict_up_of(own))
        finish(reach, jnp.where(below, rest / diagonal_of(own), rest))
        after_upper()
        for k in range(1, reach):
            acc[k - 1] = partial(k, reach - 1) - dot(low[j, k], strict_up_of(d[j + k]))
        for k in range(reach):
            wait_piece(k)
            pivot = d[j + k]
            if k == 0:
                rest = a[j, k].astype(F32) - dot(low[j, k], strict_up_of(pivot))
            else:
                rest = acc[k - 1] - dot(low[j, 0], w[j, upper(k)])
            divisor = jnp.where(mask_of(aux_own, j, k), diagonal_of(pivot), 1.0)
            finish(k, rest / divisor)

    def nothing(*_):
        pass

    def first_sweep(i, carry):
        j = rows - 1 - i

        @pl.when(from_edge)
        def _():
            remote(w1.at[j], w1.at[j], sem.at[SEND_ROWS], recv1.at[j], nxt).wait_recv()
            unpack(w1, d1, j)

        @pl.when(from_inner)
        def _():
            raw_copy(j).wait_recv()
            left = as_column(scale[j])
            for k in range(reach + 1):
                value = scaled_block(
                    h1[j, k], aux_prev, j, reach + k, left, scale[j + k]
                )
                if k == 0:
                    d1[j] = value
                else:
                    w1[j, upper(k)] = value
            farthest = w1[j, upper(reach)]
            value = farthest.astype(F32) - dot(strict_low_of(d1[j]), farthest)
            w2[j, upper(reach)] = jnp.where(mask_of(aux_prev, j, 2 * reach), value, 0.0).astype(BF16)

        def put(k, value):
            if k == reach:
                d2[reach + j] = value
            elif k > reach:
                w2[reach + j, upper(k - reach)] = value
            else:
                low2[j, k] = value

        update(j, a, w1, d1, put, nothing, nothing, nothing)

        @pl.when(has_next)
        def _():
            pack(w2, j, d2[reach + j])

        @pl.when(inner)
        def _():
            for copy, now in (
                (row_copy(j, most, j), j > 0),
                (row_copy(j, near, j), j == 0),
                (row_copy(j, third, rows), j == 0),
            ):
                pl.when(now)(copy.start)

        @pl.when(edge)
        def _():
            start(edge_copies(0, j))

        return carry

    lax.fori_loop(0, rows, first_sweep, 0)

    def hand_early():
        remote(early, early, sem.at[SEND_EARLY], early_recv.at[0], nxt).wait_recv()
        early_on().start()

    only(hands_early, hand_early)

    def pass_first(i, carry):
        pass_on(0, rows - 1 - i)
        return carry

    lax.fori_loop(0, jnp.where(jnp.logical_or(by_last, by_first), rows, 0), pass_first, 0)

    def second_sweep(i, carry):
        j = rows - 1 - i

        def put(k, value):
            f2[j, k] = value

        def before_diagonal():
            @pl.when(from_edge)
            def _():
                row_copy(j, whole, j).wait_recv()
                unpack(w2, d2, j)

        def after_upper():
            def send():
                pack(w1, j, f2[j, reach])
                for s in range(1, reach + 1):
                    w1[reach + j, upper(s)] = f2[j, reach + s]
                start(edge_copies(1, j))

            only(edge, send)
            pass_on(1, j)

        def wait_piece(k):
            if k == 0:
                @pl.when(from_inner)
                def _():
                    pl.when(j > 0)(row_copy(j, most, j).wait_recv)
                    pl.when(j == 0)(row_copy(j, near, j).wait_recv)
                    unpack(w2, d2, j)

            if k == reach - 1:
                pl.when(jnp.logical_and(from_inner, j == 0))(row_copy(j, third, rows).wait_recv)

        update(j, low2, w2, d2, put, before_diagonal, after_upper, wait_piece)
        return carry

    @pl.when(has_next)
    def _():
        to_next.wait_send()

    @pl.when(has_prev)
    def _():
        to_prev.wait_send()

    @pl.when(inner)
    def _():
        raw = blk.at[:, pl.ds(reach, reach + 1)]
        remote(raw, h1, sem.at[SEND_RAW], recv1.at[0], nxt).wait_send()

    lax.fori_loop(0, rows, second_sweep, 0)

    @pl.when(inner)
    def _():
        part = w2.at[pl.ds(reach, rows), most]
        remote(part, part, sem.at[SEND_ROWS], recv2.at[0], nxt).wait_send()

    def sent_edge():
        for t, w in enumerate((w2, w1)):
            part = w.at[pl.ds(reach, rows)]
            remote(part, part, sem.at[SEND_RAW if t else SEND_ROWS], recv2.at[0], nxt).wait_send()

    only(edge, sent_edge)

    def helped():
        remote(aside, aside, sem.at[SEND_ASIDE], recv2.at[0], nxt).wait_send()

    only(first, helped)

    @pl.when(hands_early)
    def _():
        early_on().wait_send()
    for way, duty in enumerate((by_last, by_first)):
        def passed():
            part = relay.at[:, :, pl.ds(0, ways[way].size)]
            remote(part, part, sem.at[RELAYED], recv2.at[0], nxt).wait_send()

        only(duty, passed)


def per_device(blocks, diag_shift, offsets):
    rows, band, size, _ = blocks.shape
    reach = (band - 1) // 2
    assert rows == reach == 4
    slabs, groups = lax.axis_size("slab"), lax.axis_size("grp")
    shift = diag_shift.reshape(rows, 1, size)
    block = (size, size)
    packed = size // 2 + TILE
    tall = (reach + rows, packed + reach * size, size)
    dma = pltpu.SemaphoreType.DMA
    return pl.pallas_call(
        functools.partial(kernel, slabs, groups, reach),
        out_shape=pltpu.VMEM(blocks.shape, BF16),
        in_specs=[pl.BlockSpec(memory_space=pltpu.HBM)] * 3,
        out_specs=pl.BlockSpec(memory_space=pltpu.VMEM),
        scratch_shapes=[
            pltpu.VMEM(blocks.shape, BF16),
            pltpu.VMEM((2, rows, packed + 2 * size, size), BF16),
            pltpu.VMEM((groups // SPAN - 1,) + block, BF16),
            pltpu.VMEM((EARLY,) + block, BF16),
            pltpu.SMEM((2, rows), jnp.int32),
            pltpu.VMEM((rows, 1, size), F32),
            pltpu.VMEM((AUX, size), F32),
            pltpu.VMEM((SENT, size), F32),
            pltpu.VMEM((SENT, size), F32),
            pltpu.VMEM((3 * rows, 1, size), F32),
            pltpu.VMEM(blocks.shape, BF16),
            pltpu.VMEM(tall, BF16),
            pltpu.VMEM(tall, BF16),
            pltpu.VMEM((reach + rows,) + block, BF16),
            pltpu.VMEM((reach + rows,) + block, BF16),
            pltpu.VMEM((rows, reach) + block, BF16),
            pltpu.VMEM((rows, reach + 1) + block, BF16),
            pltpu.VMEM((reach - 1,) + block, F32),
            dma((7,)), dma((2,)), dma((rows,)), dma((rows + 1,)), dma((2, rows)), dma((1,)),
            dma((1,)), pltpu.SemaphoreType.REGULAR((3,)),
        ],
        compiler_params=pltpu.CompilerParams(collective_id=0, has_side_effects=True, vmem_limit_bytes=57 << 20),
    )(blocks, shift, offsets.T)


def solution(mesh):
    return jax.shard_map(
        per_device,
        mesh=mesh,
        in_specs=(
            P(("slab", "grp"), None, None, None),
            P(("slab", "grp")),
            P(("slab", "grp"), None),
        ),
        out_specs=P(("slab", "grp"), None, None, None),
        check_vma=False,
    )
```

```python
import functools

import jax
import jax.numpy as jnp
from jax import lax
from jax.experimental import pallas as pl
from jax.experimental.pallas import tpu as pltpu
from jax.sharding import PartitionSpec as P

MESH = pl.DeviceIdType.MESH
F32 = jnp.float32
BF16 = jnp.bfloat16

DIAG, RIGHT, LEFT, SENT, AUX = 0, 4, 8, 8, 16
TILE = 8
LOAD_FIRST, LOAD_ROW, LOAD_LOWER, LOAD_SHIFT, LOAD_OFFSETS, LOAD_UPPER, LOAD_REST = range(7)
SEND_RAW, SEND_NEXT, RELAYED, SEND_ROWS, SEND_PREV, SEND_ASIDE, SEND_EARLY = range(7)
EARLY = 2
SPAN = 4


def kernel(
    slabs, groups, reach,
    blocks, shifts, offsets_in, f2,
    blk, relay, aside, early, offsets, shift_own, aux_own, aux_prev, aux_next, scale, a, w1, w2, d1, d2, low2, h1, acc,
    sem, aux_recv, recv1, recv2, relay_recv, aside_recv, early_recv, ready,
):
    rows, band, size, _ = blk.shape
    slab, grp = lax.axis_index("slab"), lax.axis_index("grp")
    here = slab * groups + grp
    has_prev = here > 0
    has_next = here < slabs * groups - 1
    after = lax.rem(here + 1, slabs * groups)
    before = lax.rem(here + slabs * groups - 1, slabs * groups)
    nxt = (lax.div(after, groups), lax.rem(after, groups))
    prv = (lax.div(before, groups), lax.rem(before, groups))
    inner = grp < groups - 1
    edge = jnp.logical_and(grp == groups - 1, has_next)
    from_inner = grp > 0
    from_edge = jnp.logical_and(grp == 0, has_prev)

    half = size // 2

    first, last = grp == 0, grp == groups - 1
    slab_above, slab_below = slab > 0, slab < slabs - 1
    by_last = jnp.logical_and(last, slab_above)
    by_first = jnp.logical_and(first, slab_below)
    slab_after = lax.rem(slab + 1, slabs)
    slab_before = lax.rem(slab + slabs - 1, slabs)
    packed = half + TILE
    diag = reach * size
    tall = diag + packed

    whole = pl.ds(0, tall)
    most = pl.ds(size, tall - size)
    near, third = pl.ds(2 * size, 2 * size + packed), pl.ds(size, size)

    def upper(s):
        return pl.ds((reach - s) * size, size)

    middle = tall // 32 * 16
    ways = (pl.ds(middle, tall - middle), pl.ds(0, middle))

    def remote(src, dst, send, recv, device):
        return pltpu.make_async_remote_copy(
            src_ref=src, dst_ref=dst, send_sem=send, recv_sem=recv,
            device_id=device, device_id_type=MESH,
        )

    def start(copies):
        for copy in copies:
            copy.start()

    def wait_send(copies):
        for copy in copies:
            copy.wait_send()

    def only(flag, body):
        def run(_, carry):
            body()
            return carry

        lax.fori_loop(0, jnp.where(flag, 1, 0), run, 0)

    def slot(t, j, way):
        return relay.at[t, j, pl.ds(0, ways[way].size)]

    def edge_copies(t, j):
        src, send = (w1, sem.at[SEND_RAW]) if t else (w2, sem.at[SEND_ROWS])
        return [
            remote(src.at[reach + j, ways[way]], slot(t, j, way), send, relay_recv.at[t, j], device)
            for way, device in enumerate(((slab_after, groups - 1), (slab, 0)))
        ]

    def forward(t, j, way):
        return remote(
            slot(t, j, way), (w2 if t else w1).at[j, ways[way]], sem.at[RELAYED],
            (recv2 if t else recv1).at[j], (slab, 0) if way == 0 else (slab_after, 0),
        )

    def pass_on(t, j):
        for way, duty in enumerate((by_last, by_first)):
            def go():
                remote(
                    slot(t, j, way), slot(t, j, way), sem.at[RELAYED], relay_recv.at[t, j], nxt
                ).wait_recv()
                forward(t, j, way).start()

            only(duty, go)

    def raw_copy(j):
        return remote(
            blk.at[j, pl.ds(reach, reach + 1)], h1.at[j], sem.at[SEND_RAW], recv1.at[j], nxt
        )

    turns = aside.shape[0]
    far = jnp.logical_and(lax.rem(grp, SPAN) == SPAN - 1, inner)
    from_far = jnp.logical_and(lax.rem(grp, SPAN) == 0, grp > 0)
    odd = lax.rem(grp, 2) == 1
    even = jnp.logical_not(odd)
    odd_inner, even_inner = jnp.logical_and(odd, inner), jnp.logical_and(even, inner)
    odd_near = jnp.logical_and(odd_inner, jnp.logical_not(far))
    hands_early = jnp.logical_and(odd, grp > 2)
    here_on = pl.ds(0, EARLY)
    odd_after = (slab, lax.rem(grp + 2, groups))

    def raw_early():
        return remote(
            blk.at[0, pl.ds(reach, EARLY)], early, sem.at[SEND_RAW], early_recv.at[0], odd_after
        )

    def early_on():
        return remote(early, h1.at[0, here_on], sem.at[SEND_EARLY], recv1.at[0], prv)

    def raw_aside():
        turn = lax.div(grp, SPAN)
        return remote(
            blk.at[0, 2 * reach], aside.at[turn], sem.at[SEND_RAW], aside_recv.at[0], (slab, 0)
        )

    def raw_straight(blocks_left):
        return remote(
            blk.at[0, pl.ds(reach + EARLY, blocks_left)], h1.at[0, pl.ds(EARLY, blocks_left)],
            sem.at[SEND_RAW], recv1.at[0], nxt,
        )

    def help_on(turn):
        return remote(
            aside.at[turn], h1.at[0, reach], sem.at[SEND_ASIDE], recv1.at[0], (slab, SPAN * (turn + 1))
        )

    def row_copy(j, part, arrived):
        return remote(w2.at[reach + j, part], w2.at[j, part], sem.at[SEND_ROWS], recv2.at[arrived], nxt)

    def load(which, rows_of, cut_of):
        return pltpu.make_async_copy(
            blocks.at[rows_of, cut_of], blk.at[rows_of, cut_of], sem.at[which]
        )

    above_cut = pl.ds(reach, reach + 1)
    load_first = load(LOAD_FIRST, pl.ds(0, 1), pl.ds(reach, EARLY))
    load_row = load(LOAD_ROW, pl.ds(rows - 1, 1), above_cut)
    load_upper = load(LOAD_UPPER, pl.ds(1, rows - 2), above_cut)
    load_rest = load(LOAD_REST, pl.ds(0, 1), pl.ds(reach + EARLY, reach + 1 - EARLY))
    load_lower = load(LOAD_LOWER, pl.ds(0, rows), pl.ds(0, reach))
    load_shift = pltpu.make_async_copy(shifts, shift_own, sem.at[LOAD_SHIFT])
    load_offsets = pltpu.make_async_copy(offsets_in, offsets, sem.at[LOAD_OFFSETS])

    to_next = remote(aux_own.at[pl.ds(0, SENT)], aux_prev, sem.at[SEND_NEXT], aux_recv.at[0], nxt)
    to_prev = remote(aux_own.at[pl.ds(0, SENT)], aux_next, sem.at[SEND_PREV], aux_recv.at[1], prv)

    barrier = pltpu.get_barrier_semaphore()

    def greet(flag, device):
        @pl.when(flag)
        def _():
            pl.semaphore_signal(barrier, inc=1, device_id=device, device_id_type=MESH)

    def tell(flag, n, device):
        @pl.when(flag)
        def _():
            pl.semaphore_signal(ready.at[n], inc=1, device_id=device, device_id_type=MESH)

    both = jnp.logical_and
    corner = both(jnp.logical_or(first, last), slabs > 1)
    greet(hands_early, (slab, lax.rem(grp + groups - 2, groups)))
    greet(both(odd, has_next), nxt)
    greet(odd, prv)

    load_first.start()
    load_row.start()
    load_shift.start()
    load_offsets.start()
    load_upper.start()
    load_rest.start()
    load_lower.start()

    greet(both(last, slabs > 1), (slab, 0))
    greet(both(corner, slab_below), (slab_after, grp))
    greet(both(corner, slab_above), (slab_before, grp))
    greet(jnp.logical_or(far, from_far), (slab, 0))

    def count(*flags):
        return sum(flag.astype(jnp.int32) for flag in flags)

    around = count(corner) * count(slab_below, slab_above)
    mine = count(odd_inner) + around
    theirs = count(has_prev) + 1 + count(both(first, slabs > 1)) + around + 2 * turns * count(first)
    peers = jnp.where(odd, mine, theirs)
    pl.semaphore_wait(barrier, peers)

    @pl.when(odd_inner)
    def _():
        load_first.wait()
        raw_early().start()

    tell(both(even, has_prev), 0, prv)
    tell(even, 2, nxt)
    tell(both(first, slabs > 1), 2, (slab, groups - 1))
    for turn in range(turns):
        tell(first, 1, (slab, SPAN * turn + SPAN - 1))
    pl.when(jnp.logical_not(odd_inner))(load_first.wait)
    load_row.wait()

    @pl.when(both(odd, has_next))
    def _():
        pl.semaphore_wait(ready.at[0], 1)

    @pl.when(inner)
    def _():
        raw_copy(rows - 1).start()

    row_id = lax.broadcasted_iota(jnp.int32, (size, size), 0)
    col_id = lax.broadcasted_iota(jnp.int32, (size, size), 1)
    eye = row_id == col_id

    def scale_of(values):
        positive = values > 0
        return jnp.where(positive, 1.0 / jnp.sqrt(jnp.where(positive, values, 1.0)), 0.0)

    def as_column(row):
        return jnp.sum(jnp.where(eye, row, 0.0), axis=1, keepdims=True)

    @pl.when(jnp.logical_not(has_prev))
    def _():
        aux_prev[...] = jnp.zeros_like(aux_prev)
        for w, d in ((w1, d1), (w2, d2)):
            for j in range(reach):
                w[j] = jnp.zeros((tall, size), BF16)
                d[j] = jnp.zeros((size, size), BF16)

    @pl.when(jnp.logical_not(has_next))
    def _():
        aux_next[...] = jnp.zeros_like(aux_next)

    load_shift.wait()
    load_offsets.wait()
    load_upper.wait()
    load_rest.wait()
    for j in range(rows):
        diagonal = jnp.sum(
            jnp.where(eye, blk[j, reach].astype(F32), 0.0), axis=0, keepdims=True
        )
        aux_own[DIAG + j : DIAG + j + 1, :] = shift_own[j] + diagonal
        row = here * rows + j
        right = jnp.minimum(offsets[1, j], slabs * groups * rows - 1 - row)
        left = jnp.minimum(offsets[0, j], row)
        aux_own[RIGHT + j : RIGHT + j + 1, :] = jnp.full((1, size), right, jnp.int32).astype(F32)
        aux_own[LEFT + j : LEFT + j + 1, :] = jnp.full((1, size), left, jnp.int32).astype(F32)

    @pl.when(has_next)
    def _():
        to_next.start()

    @pl.when(inner)
    def _():
        for j in reversed(range(1, rows - 1)):
            raw_copy(j).start()

    @pl.when(even_inner)
    def _():
        raw_copy(0).start()

    @pl.when(odd_near)
    def _():
        raw_straight(reach + 1 - EARLY).start()

    @pl.when(far)
    def _():
        raw_straight(reach - EARLY).start()

    @pl.when(odd)
    def _():
        pl.semaphore_wait(ready.at[2], 1 + count(both(last, slabs > 1)))

    @pl.when(has_prev)
    def _():
        to_prev.start()

    @pl.when(has_prev)
    def _():
        to_next.wait_recv()

    @pl.when(has_next)
    def _():
        to_prev.wait_recv()

    for j in range(rows):
        scale[j] = scale_of(aux_prev[DIAG + j : DIAG + j + 1, :])
        scale[rows + j] = scale_of(aux_own[DIAG + j : DIAG + j + 1, :])
        scale[2 * rows + j] = scale_of(aux_next[DIAG + j : DIAG + j + 1, :])

    def mask_of(table, j, k):
        place, away = (RIGHT, k - reach) if k >= reach else (LEFT, reach - k)
        return table[pl.ds(place + j, 1), :] >= away

    def scaled_block(block, table, j, k, left, right):
        value = block.astype(F32)
        if k == reach:
            value = jnp.where(eye, table[pl.ds(DIAG + j, 1), :], value)
        value = value * left * right
        if k != reach:
            value = jnp.where(mask_of(table, j, k), value, 0.0)
        return value.astype(BF16)

    def scale_own(j, carry):
        left = as_column(scale[rows + j])
        for k in range(band):
            value = scaled_block(blk[j, k], aux_own, j, k, left, scale[j + k])
            a[j, k] = value
            if k == reach:
                d1[reach + j] = value
            elif k > reach:
                w1[reach + j, upper(k - reach)] = value
        return carry

    load_lower.wait()
    lax.fori_loop(0, rows, scale_own, 0)

    @pl.when(far)
    def _():
        pl.semaphore_wait(ready.at[1], 1)
        raw_aside().start()

    def help_all():
        remote(aside, aside, sem.at[SEND_ASIDE], aside_recv.at[0], nxt).wait_recv()
        for turn in range(turns):
            help_on(turn).start()

    only(first, help_all)

    below = row_id > col_id

    def dot(x, y):
        return jnp.dot(x, y, preferred_element_type=F32)

    def strict_low_of(block):
        return jnp.where(below, block.astype(F32), 0.0).astype(BF16)

    def strict_up_of(block):
        return jnp.where(row_id < col_id, block.astype(F32), 0.0).astype(BF16)

    def diagonal_of(block):
        return jnp.sum(jnp.where(eye, block.astype(F32), 0.0), axis=0, keepdims=True)

    above = lax.broadcasted_iota(jnp.int32, (half, half), 0) < lax.broadcasted_iota(jnp.int32, (half, half), 1)

    def pack(w, j, block):
        top, corner = block[0:half, 0:half], block[half:size, half:size]
        both = jnp.where(above, top.astype(F32), corner.astype(F32).T)
        w[reach + j, diag : diag + half, 0:half] = both.astype(BF16)
        w[reach + j, diag : diag + half, half:size] = block[0:half, half:size]
        w[reach + j, diag + half : tall, :] = jnp.broadcast_to(diagonal_of(block), (TILE, size)).astype(BF16)

    def unpack(w, d, j):
        both = w[j, diag : diag + half, 0:half].astype(F32)
        diagonal = w[j, diag + half : tall, :].astype(F32)[0:1]
        on = eye[0:half, 0:half]
        for n, part in enumerate((both, both.T)):
            place = slice(n * half, (n + 1) * half)
            value = jnp.where(above, part, 0.0) + jnp.where(on, diagonal[:, place], 0.0)
            d[j, place, place] = value.astype(BF16)
        d[j, 0:half, half:size] = w[j, diag : diag + half, half:size]

    def update(j, low, w, d, put, before_diagonal, after_upper, wait_piece):
        def partial(k, most):
            total = a[j, k].astype(F32)
            for m in range(1, most + 1):
                s = k - reach + m
                if 1 <= s <= reach:
                    total = total - dot(low[j, reach - m], w[reach + j - m, upper(s)])
            return total

        def finish(k, value):
            if k != reach:
                value = jnp.where(mask_of(aux_own, j, k), value, 0.0)
            put(k, value.astype(BF16))

        own = d[reach + j]
        strict_low = strict_low_of(own)
        for k in range(reach + 1, band):
            finish(k, partial(k, reach) - dot(strict_low, w[reach + j, upper(k - reach)]))
        before_diagonal()
        rest = partial(reach, reach) - dot(strict_low, strict_up_of(own))
        finish(reach, jnp.where(below, rest / diagonal_of(own), rest))
        after_upper()
        for k in range(1, reach):
            acc[k - 1] = partial(k, reach - 1) - dot(low[j, k], strict_up_of(d[j + k]))
        for k in range(reach):
            wait_piece(k)
            pivot = d[j + k]
            if k == 0:
                rest = a[j, k].astype(F32) - dot(low[j, k], strict_up_of(pivot))
            else:
                rest = acc[k - 1] - dot(low[j, 0], w[j, upper(k)])
            divisor = jnp.where(mask_of(aux_own, j, k), diagonal_of(pivot), 1.0)
            finish(k, rest / divisor)

    def nothing(*_):
        pass

    def first_sweep(i, carry):
        j = rows - 1 - i

        @pl.when(from_edge)
        def _():
            remote(w1.at[j], w1.at[j], sem.at[SEND_ROWS], recv1.at[j], nxt).wait_recv()
            unpack(w1, d1, j)

        @pl.when(from_inner)
        def _():
            raw_copy(j).wait_recv()
            left = as_column(scale[j])
            for k in range(reach + 1):
                value = scaled_block(
                    h1[j, k], aux_prev, j, reach + k, left, scale[j + k]
                )
                if k == 0:
                    d1[j] = value
                else:
                    w1[j, upper(k)] = value
            farthest = w1[j, upper(reach)]
            value = farthest.astype(F32) - dot(strict_low_of(d1[j]), farthest)
            w2[j, upper(reach)] = jnp.where(mask_of(aux_prev, j, 2 * reach), value, 0.0).astype(BF16)

        def put(k, value):
            if k == reach:
                d2[reach + j] = value
            elif k > reach:
                w2[reach + j, upper(k - reach)] = value
            else:
                low2[j, k] = value

        update(j, a, w1, d1, put, nothing, nothing, nothing)

        @pl.when(has_next)
        def _():
            pack(w2, j, d2[reach + j])

        @pl.when(inner)
        def _():
            for copy, now in (
                (row_copy(j, most, j), j > 0),
                (row_copy(j, near, j), j == 0),
                (row_copy(j, third, rows), j == 0),
            ):
                pl.when(now)(copy.start)

        @pl.when(edge)
        def _():
            start(edge_copies(0, j))

        return carry

    lax.fori_loop(0, rows, first_sweep, 0)

    def hand_early():
        remote(early, early, sem.at[SEND_EARLY], early_recv.at[0], nxt).wait_recv()
        early_on().start()

    only(hands_early, hand_early)

    def pass_first(i, carry):
        pass_on(0, rows - 1 - i)
        return carry

    lax.fori_loop(0, jnp.where(jnp.logical_or(by_last, by_first), rows, 0), pass_first, 0)

    def second_sweep(i, carry):
        j = rows - 1 - i

        def put(k, value):
            f2[j, k] = value

        def before_diagonal():
            @pl.when(from_edge)
            def _():
                row_copy(j, whole, j).wait_recv()
                unpack(w2, d2, j)

        def after_upper():
            def send():
                pack(w1, j, f2[j, reach])
                for s in range(1, reach + 1):
                    w1[reach + j, upper(s)] = f2[j, reach + s]
                start(edge_copies(1, j))

            only(edge, send)
            pass_on(1, j)

        def wait_piece(k):
            if k == 0:
                @pl.when(from_inner)
                def _():
                    pl.when(j > 0)(row_copy(j, most, j).wait_recv)
                    pl.when(j == 0)(row_copy(j, near, j).wait_recv)
                    unpack(w2, d2, j)

            if k == reach - 1:
                pl.when(jnp.logical_and(from_inner, j == 0))(row_copy(j, third, rows).wait_recv)

        update(j, low2, w2, d2, put, before_diagonal, after_upper, wait_piece)
        return carry

    @pl.when(has_next)
    def _():
        to_next.wait_send()

    @pl.when(has_prev)
    def _():
        to_prev.wait_send()

    @pl.when(inner)
    def _():
        raw = blk.at[:, pl.ds(reach, reach + 1)]
        remote(raw, h1, sem.at[SEND_RAW], recv1.at[0], nxt).wait_send()

    lax.fori_loop(0, rows, second_sweep, 0)

    @pl.when(inner)
    def _():
        part = w2.at[pl.ds(reach, rows), most]
        remote(part, part, sem.at[SEND_ROWS], recv2.at[0], nxt).wait_send()

    def sent_edge():
        for t, w in enumerate((w2, w1)):
            part = w.at[pl.ds(reach, rows)]
            remote(part, part, sem.at[SEND_RAW if t else SEND_ROWS], recv2.at[0], nxt).wait_send()

    only(edge, sent_edge)

    def helped():
        remote(aside, aside, sem.at[SEND_ASIDE], recv2.at[0], nxt).wait_send()

    only(first, helped)

    @pl.when(hands_early)
    def _():
        early_on().wait_send()
    for way, duty in enumerate((by_last, by_first)):
        def passed():
            part = relay.at[:, :, pl.ds(0, ways[way].size)]
            remote(part, part, sem.at[RELAYED], recv2.at[0], nxt).wait_send()

        only(duty, passed)


def per_device(blocks, diag_shift, offsets):
    rows, band, size, _ = blocks.shape
    reach = (band - 1) // 2
    assert rows == reach == 4
    slabs, groups = lax.axis_size("slab"), lax.axis_size("grp")
    shift = diag_shift.reshape(rows, 1, size)
    block = (size, size)
    packed = size // 2 + TILE
    tall = (reach + rows, packed + reach * size, size)
    dma = pltpu.SemaphoreType.DMA
    return pl.pallas_call(
        functools.partial(kernel, slabs, groups, reach),
        out_shape=pltpu.VMEM(blocks.shape, BF16),
        in_specs=[pl.BlockSpec(memory_space=pltpu.HBM)] * 3,
        out_specs=pl.BlockSpec(memory_space=pltpu.VMEM),
        scratch_shapes=[
            pltpu.VMEM(blocks.shape, BF16),
            pltpu.VMEM((2, rows, packed + 2 * size, size), BF16),
            pltpu.VMEM((groups // SPAN - 1,) + block, BF16),
            pltpu.VMEM((EARLY,) + block, BF16),
            pltpu.SMEM((2, rows), jnp.int32),
            pltpu.VMEM((rows, 1, size), F32),
            pltpu.VMEM((AUX, size), F32),
            pltpu.VMEM((SENT, size), F32),
            pltpu.VMEM((SENT, size), F32),
            pltpu.VMEM((3 * rows, 1, size), F32),
            pltpu.VMEM(blocks.shape, BF16),
            pltpu.VMEM(tall, BF16),
            pltpu.VMEM(tall, BF16),
            pltpu.VMEM((reach + rows,) + block, BF16),
            pltpu.VMEM((reach + rows,) + block, BF16),
            pltpu.VMEM((rows, reach) + block, BF16),
            pltpu.VMEM((rows, reach + 1) + block, BF16),
            pltpu.VMEM((reach - 1,) + block, F32),
            dma((7,)), dma((2,)), dma((rows,)), dma((rows + 1,)), dma((2, rows)), dma((1,)),
            dma((1,)), pltpu.SemaphoreType.REGULAR((3,)),
        ],
        compiler_params=pltpu.CompilerParams(collective_id=0, has_side_effects=True, vmem_limit_bytes=57 << 20),
    )(blocks, shift, offsets.T)


def solution(mesh):
    return jax.shard_map(
        per_device,
        mesh=mesh,
        in_specs=(
            P(("slab", "grp"), None, None, None),
            P(("slab", "grp")),
            P(("slab", "grp"), None),
        ),
        out_specs=P(("slab", "grp"), None, None, None),
        check_vma=False,
    )
```

```python
import functools

import jax
import jax.numpy as jnp
from jax import lax
from jax.experimental import pallas as pl
from jax.experimental.pallas import tpu as pltpu
from jax.sharding import PartitionSpec as P

MESH = pl.DeviceIdType.MESH
F32 = jnp.float32
BF16 = jnp.bfloat16

DIAG, RIGHT, LEFT, SENT, AUX = 0, 4, 8, 8, 16
TILE = 8
LOAD_FIRST, LOAD_ROW, LOAD_LOWER, LOAD_SHIFT, LOAD_OFFSETS, LOAD_UPPER, LOAD_REST = range(7)
SEND_RAW, SEND_NEXT, RELAYED, SEND_ROWS, SEND_PREV, SEND_ASIDE, SEND_EARLY = range(7)
EARLY = 2
SPAN = 4


def kernel(
    slabs, groups, reach,
    blocks, shifts, offsets_in, f2,
    blk, relay, aside, early, offsets, shift_own, aux_own, aux_prev, aux_next, scale, a, w1, w2, d1, d2, low2, h1, acc,
    sem, aux_recv, recv1, recv2, relay_recv, side_recv, ready,
):
    rows, band, size, _ = blk.shape
    slab, grp = lax.axis_index("slab"), lax.axis_index("grp")
    here = slab * groups + grp
    has_prev = here > 0
    has_next = here < slabs * groups - 1
    after = lax.rem(here + 1, slabs * groups)
    before = lax.rem(here + slabs * groups - 1, slabs * groups)
    nxt = (lax.div(after, groups), lax.rem(after, groups))
    prv = (lax.div(before, groups), lax.rem(before, groups))
    inner = grp < groups - 1
    edge = jnp.logical_and(grp == groups - 1, has_next)
    from_inner = grp > 0
    from_edge = jnp.logical_and(grp == 0, has_prev)

    half = size // 2

    first, last = grp == 0, grp == groups - 1
    slab_above, slab_below = slab > 0, slab < slabs - 1
    by_last = jnp.logical_and(last, slab_above)
    by_first = jnp.logical_and(first, slab_below)
    slab_after = lax.rem(slab + 1, slabs)
    slab_before = lax.rem(slab + slabs - 1, slabs)
    packed = half + TILE
    diag = reach * size
    tall = diag + packed

    whole = pl.ds(0, tall)
    most = pl.ds(size, tall - size)
    near, third = pl.ds(2 * size, 2 * size + packed), pl.ds(size, size)

    def upper(s):
        return pl.ds((reach - s) * size, size)

    middle = tall // 32 * 16
    ways = (pl.ds(middle, tall - middle), pl.ds(0, middle))

    def remote(src, dst, send, recv, device):
        return pltpu.make_async_remote_copy(
            src_ref=src, dst_ref=dst, send_sem=send, recv_sem=recv,
            device_id=device, device_id_type=MESH,
        )

    def start(copies):
        for copy in copies:
            copy.start()

    def wait_send(copies):
        for copy in copies:
            copy.wait_send()

    def only(flag, body):
        def run(_, carry):
            body()
            return carry

        lax.fori_loop(0, jnp.where(flag, 1, 0), run, 0)

    def slot(t, j, way):
        return relay.at[t, j, pl.ds(0, ways[way].size)]

    def edge_copies(t, j):
        src, send = (w1, sem.at[SEND_RAW]) if t else (w2, sem.at[SEND_ROWS])
        return [
            remote(src.at[reach + j, ways[way]], slot(t, j, way), send, relay_recv.at[t, j], device)
            for way, device in enumerate(((slab_after, groups - 1), (slab, 0)))
        ]

    def forward(t, j, way):
        return remote(
            slot(t, j, way), (w2 if t else w1).at[j, ways[way]], sem.at[RELAYED],
            (recv2 if t else recv1).at[j], (slab, 0) if way == 0 else (slab_after, 0),
        )

    def pass_on(t, j):
        for way, duty in enumerate((by_last, by_first)):
            def go():
                remote(
                    slot(t, j, way), slot(t, j, way), sem.at[RELAYED], relay_recv.at[t, j], nxt
                ).wait_recv()
                forward(t, j, way).start()

            only(duty, go)

    def raw_copy(j):
        return remote(
            blk.at[j, pl.ds(reach, reach + 1)], h1.at[j], sem.at[SEND_RAW], recv1.at[j], nxt
        )

    turns = aside.shape[0]
    far = jnp.logical_and(lax.rem(grp, SPAN) == SPAN - 1, inner)
    from_far = jnp.logical_and(lax.rem(grp, SPAN) == 0, grp > 0)
    odd = lax.rem(grp, 2) == 1
    even = jnp.logical_not(odd)
    odd_inner, even_inner = jnp.logical_and(odd, inner), jnp.logical_and(even, inner)
    odd_near = jnp.logical_and(odd_inner, jnp.logical_not(far))
    hands_early = jnp.logical_and(odd, grp > 2)
    here_on = pl.ds(0, EARLY)
    odd_after = (slab, lax.rem(grp + 2, groups))

    def raw_early():
        return remote(
            blk.at[0, pl.ds(reach, EARLY)], early, sem.at[SEND_RAW], side_recv.at[0], odd_after
        )

    def early_on():
        return remote(early, h1.at[0, here_on], sem.at[SEND_EARLY], recv1.at[0], prv)

    def raw_aside():
        turn = lax.div(grp, SPAN)
        return remote(
            blk.at[0, 2 * reach], aside.at[turn], sem.at[SEND_RAW], side_recv.at[0], (slab, 0)
        )

    def raw_straight(blocks_left):
        return remote(
            blk.at[0, pl.ds(reach + EARLY, blocks_left)], h1.at[0, pl.ds(EARLY, blocks_left)],
            sem.at[SEND_RAW], recv1.at[0], nxt,
        )

    def help_on(turn):
        return remote(
            aside.at[turn], h1.at[0, reach], sem.at[SEND_ASIDE], recv1.at[0], (slab, SPAN * (turn + 1))
        )

    def row_copy(j, part, arrived):
        return remote(w2.at[reach + j, part], w2.at[j, part], sem.at[SEND_ROWS], recv2.at[arrived], nxt)

    def load(which, rows_of, cut_of):
        return pltpu.make_async_copy(
            blocks.at[rows_of, cut_of], blk.at[rows_of, cut_of], sem.at[which]
        )

    above_cut = pl.ds(reach, reach + 1)
    load_first = load(LOAD_FIRST, pl.ds(0, 1), pl.ds(reach, EARLY))
    load_row = load(LOAD_ROW, pl.ds(rows - 1, 1), above_cut)
    load_upper = load(LOAD_UPPER, pl.ds(1, rows - 2), above_cut)
    load_rest = load(LOAD_REST, pl.ds(0, 1), pl.ds(reach + EARLY, reach + 1 - EARLY))
    load_lower = load(LOAD_LOWER, pl.ds(0, rows), pl.ds(0, reach))
    load_shift = pltpu.make_async_copy(shifts, shift_own, sem.at[LOAD_SHIFT])
    load_offsets = pltpu.make_async_copy(offsets_in, offsets, sem.at[LOAD_OFFSETS])

    to_next = remote(aux_own.at[pl.ds(0, SENT)], aux_prev, sem.at[SEND_NEXT], aux_recv.at[0], nxt)
    to_prev = remote(aux_own.at[pl.ds(0, SENT)], aux_next, sem.at[SEND_PREV], aux_recv.at[1], prv)

    barrier = pltpu.get_barrier_semaphore()

    def greet(flag, device):
        @pl.when(flag)
        def _():
            pl.semaphore_signal(barrier, inc=1, device_id=device, device_id_type=MESH)

    def tell(flag, n, device):
        @pl.when(flag)
        def _():
            pl.semaphore_signal(ready.at[n], inc=1, device_id=device, device_id_type=MESH)

    both = jnp.logical_and
    corner = both(jnp.logical_or(first, last), slabs > 1)
    greet(hands_early, (slab, lax.rem(grp + groups - 2, groups)))
    greet(both(odd, has_next), nxt)
    greet(odd, prv)

    load_first.start()
    load_row.start()
    load_shift.start()
    load_offsets.start()
    load_upper.start()
    load_rest.start()
    load_lower.start()

    greet(both(last, slabs > 1), (slab, 0))
    greet(both(corner, slab_below), (slab_after, grp))
    greet(both(corner, slab_above), (slab_before, grp))
    greet(jnp.logical_or(far, from_far), (slab, 0))

    def count(*flags):
        return sum(flag.astype(jnp.int32) for flag in flags)

    around = count(corner) * count(slab_below, slab_above)
    mine = count(odd_inner) + around
    theirs = count(has_prev) + 1 + count(both(first, slabs > 1)) + around + 2 * turns * count(first)
    peers = jnp.where(odd, mine, theirs)
    pl.semaphore_wait(barrier, peers)

    @pl.when(odd_inner)
    def _():
        load_first.wait()
        raw_early().start()

    tell(both(even, has_prev), 0, prv)
    tell(even, 2, nxt)
    tell(both(first, slabs > 1), 2, (slab, groups - 1))
    for turn in range(turns):
        tell(first, 1, (slab, SPAN * turn + SPAN - 1))
    pl.when(jnp.logical_not(odd_inner))(load_first.wait)
    load_row.wait()

    @pl.when(both(odd, has_next))
    def _():
        pl.semaphore_wait(ready.at[0], 1)

    @pl.when(inner)
    def _():
        raw_copy(rows - 1).start()

    row_id = lax.broadcasted_iota(jnp.int32, (size, size), 0)
    col_id = lax.broadcasted_iota(jnp.int32, (size, size), 1)
    eye = row_id == col_id

    def scale_of(values):
        positive = values > 0
        return jnp.where(positive, 1.0 / jnp.sqrt(jnp.where(positive, values, 1.0)), 0.0)

    def as_column(row):
        return jnp.sum(jnp.where(eye, row, 0.0), axis=1, keepdims=True)

    @pl.when(jnp.logical_not(has_prev))
    def _():
        aux_prev[...] = jnp.zeros_like(aux_prev)
        for w, d in ((w1, d1), (w2, d2)):
            for j in range(reach):
                w[j] = jnp.zeros((tall, size), BF16)
                d[j] = jnp.zeros((size, size), BF16)

    @pl.when(jnp.logical_not(has_next))
    def _():
        aux_next[...] = jnp.zeros_like(aux_next)

    load_shift.wait()
    load_offsets.wait()
    load_upper.wait()
    load_rest.wait()
    for j in range(rows):
        diagonal = jnp.sum(
            jnp.where(eye, blk[j, reach].astype(F32), 0.0), axis=0, keepdims=True
        )
        aux_own[DIAG + j : DIAG + j + 1, :] = shift_own[j] + diagonal
        row = here * rows + j
        right = jnp.minimum(offsets[1, j], slabs * groups * rows - 1 - row)
        left = jnp.minimum(offsets[0, j], row)
        aux_own[RIGHT + j : RIGHT + j + 1, :] = jnp.full((1, size), right, jnp.int32).astype(F32)
        aux_own[LEFT + j : LEFT + j + 1, :] = jnp.full((1, size), left, jnp.int32).astype(F32)

    @pl.when(has_next)
    def _():
        to_next.start()

    @pl.when(inner)
    def _():
        for j in reversed(range(1, rows - 1)):
            raw_copy(j).start()

    @pl.when(even_inner)
    def _():
        raw_copy(0).start()

    @pl.when(odd_near)
    def _():
        raw_straight(reach + 1 - EARLY).start()

    @pl.when(far)
    def _():
        raw_straight(reach - EARLY).start()

    @pl.when(odd)
    def _():
        pl.semaphore_wait(ready.at[2], 1 + count(both(last, slabs > 1)))

    @pl.when(has_prev)
    def _():
        to_prev.start()

    @pl.when(has_prev)
    def _():
        to_next.wait_recv()

    @pl.when(has_next)
    def _():
        to_prev.wait_recv()

    for j in range(rows):
        scale[j] = scale_of(aux_prev[DIAG + j : DIAG + j + 1, :])
        scale[rows + j] = scale_of(aux_own[DIAG + j : DIAG + j + 1, :])
        scale[2 * rows + j] = scale_of(aux_next[DIAG + j : DIAG + j + 1, :])

    def mask_of(table, j, k):
        place, away = (RIGHT, k - reach) if k >= reach else (LEFT, reach - k)
        return table[pl.ds(place + j, 1), :] >= away

    def scaled_block(block, table, j, k, left, right):
        value = block.astype(F32)
        if k == reach:
            value = jnp.where(eye, table[pl.ds(DIAG + j, 1), :], value)
        value = value * left * right
        if k != reach:
            value = jnp.where(mask_of(table, j, k), value, 0.0)
        return value.astype(BF16)

    def scale_own(j, carry):
        left = as_column(scale[rows + j])
        for k in range(band):
            value = scaled_block(blk[j, k], aux_own, j, k, left, scale[j + k])
            a[j, k] = value
            if k == reach:
                d1[reach + j] = value
            elif k > reach:
                w1[reach + j, upper(k - reach)] = value
        return carry

    load_lower.wait()
    lax.fori_loop(0, rows, scale_own, 0)

    @pl.when(far)
    def _():
        pl.semaphore_wait(ready.at[1], 1)
        raw_aside().start()

    def help_all():
        remote(aside, aside, sem.at[SEND_ASIDE], side_recv.at[0], nxt).wait_recv()
        for turn in range(turns):
            help_on(turn).start()

    only(first, help_all)

    below = row_id > col_id

    def dot(x, y):
        return jnp.dot(x, y, preferred_element_type=F32)

    def strict_low_of(block):
        return jnp.where(below, block.astype(F32), 0.0).astype(BF16)

    def strict_up_of(block):
        return jnp.where(row_id < col_id, block.astype(F32), 0.0).astype(BF16)

    def diagonal_of(block):
        return jnp.sum(jnp.where(eye, block.astype(F32), 0.0), axis=0, keepdims=True)

    above = lax.broadcasted_iota(jnp.int32, (half, half), 0) < lax.broadcasted_iota(jnp.int32, (half, half), 1)

    def pack(w, j, block):
        top, corner = block[0:half, 0:half], block[half:size, half:size]
        both = jnp.where(above, top.astype(F32), corner.astype(F32).T)
        w[reach + j, diag : diag + half, 0:half] = both.astype(BF16)
        w[reach + j, diag : diag + half, half:size] = block[0:half, half:size]
        w[reach + j, diag + half : tall, :] = jnp.broadcast_to(diagonal_of(block), (TILE, size)).astype(BF16)

    def unpack(w, d, j):
        both = w[j, diag : diag + half, 0:half].astype(F32)
        diagonal = w[j, diag + half : tall, :].astype(F32)[0:1]
        on = eye[0:half, 0:half]
        for n, part in enumerate((both, both.T)):
            place = slice(n * half, (n + 1) * half)
            value = jnp.where(above, part, 0.0) + jnp.where(on, diagonal[:, place], 0.0)
            d[j, place, place] = value.astype(BF16)
        d[j, 0:half, half:size] = w[j, diag : diag + half, half:size]

    def update(j, low, w, d, put, before_diagonal, after_upper, wait_piece):
        def partial(k, most):
            total = a[j, k].astype(F32)
            for m in range(1, most + 1):
                s = k - reach + m
                if 1 <= s <= reach:
                    total = total - dot(low[j, reach - m], w[reach + j - m, upper(s)])
            return total

        def finish(k, value):
            if k != reach:
                value = jnp.where(mask_of(aux_own, j, k), value, 0.0)
            put(k, value.astype(BF16))

        own = d[reach + j]
        strict_low = strict_low_of(own)
        for k in range(reach + 1, band):
            finish(k, partial(k, reach) - dot(strict_low, w[reach + j, upper(k - reach)]))
        before_diagonal()
        rest = partial(reach, reach) - dot(strict_low, strict_up_of(own))
        finish(reach, jnp.where(below, rest / diagonal_of(own), rest))
        after_upper()
        for k in range(1, reach):
            acc[k - 1] = partial(k, reach - 1) - dot(low[j, k], strict_up_of(d[j + k]))
        for k in range(reach):
            wait_piece(k)
            pivot = d[j + k]
            if k == 0:
                rest = a[j, k].astype(F32) - dot(low[j, k], strict_up_of(pivot))
            else:
                rest = acc[k - 1] - dot(low[j, 0], w[j, upper(k)])
            divisor = jnp.where(mask_of(aux_own, j, k), diagonal_of(pivot), 1.0)
            finish(k, rest / divisor)

    def nothing(*_):
        pass

    def first_sweep(i, carry):
        j = rows - 1 - i

        @pl.when(from_edge)
        def _():
            remote(w1.at[j], w1.at[j], sem.at[SEND_ROWS], recv1.at[j], nxt).wait_recv()
            unpack(w1, d1, j)

        @pl.when(from_inner)
        def _():
            raw_copy(j).wait_recv()
            left = as_column(scale[j])
            for k in range(reach + 1):
                value = scaled_block(
                    h1[j, k], aux_prev, j, reach + k, left, scale[j + k]
                )
                if k == 0:
                    d1[j] = value
                else:
                    w1[j, upper(k)] = value
            farthest = w1[j, upper(reach)]
            value = farthest.astype(F32) - dot(strict_low_of(d1[j]), farthest)
            w2[j, upper(reach)] = jnp.where(mask_of(aux_prev, j, 2 * reach), value, 0.0).astype(BF16)

        def put(k, value):
            if k == reach:
                d2[reach + j] = value
            elif k > reach:
                w2[reach + j, upper(k - reach)] = value
            else:
                low2[j, k] = value

        update(j, a, w1, d1, put, nothing, nothing, nothing)

        @pl.when(has_next)
        def _():
            pack(w2, j, d2[reach + j])

        @pl.when(inner)
        def _():
            for copy, now in (
                (row_copy(j, most, j), j > 0),
                (row_copy(j, near, j), j == 0),
                (row_copy(j, third, rows), j == 0),
            ):
                pl.when(now)(copy.start)

        @pl.when(edge)
        def _():
            start(edge_copies(0, j))

        return carry

    lax.fori_loop(0, rows, first_sweep, 0)

    def hand_early():
        remote(early, early, sem.at[SEND_EARLY], side_recv.at[0], nxt).wait_recv()
        early_on().start()

    only(hands_early, hand_early)

    def pass_first(i, carry):
        pass_on(0, rows - 1 - i)
        return carry

    lax.fori_loop(0, jnp.where(jnp.logical_or(by_last, by_first), rows, 0), pass_first, 0)

    def second_sweep(i, carry):
        j = rows - 1 - i

        def put(k, value):
            f2[j, k] = value

        def before_diagonal():
            @pl.when(from_edge)
            def _():
                row_copy(j, whole, j).wait_recv()
                unpack(w2, d2, j)

        def after_upper():
            def send():
                pack(w1, j, f2[j, reach])
                for s in range(1, reach + 1):
                    w1[reach + j, upper(s)] = f2[j, reach + s]
                start(edge_copies(1, j))

            only(edge, send)
            pass_on(1, j)

        def wait_piece(k):
            if k == 0:
                @pl.when(from_inner)
                def _():
                    pl.when(j > 0)(row_copy(j, most, j).wait_recv)
                    pl.when(j == 0)(row_copy(j, near, j).wait_recv)
                    unpack(w2, d2, j)

            if k == reach - 1:
                pl.when(jnp.logical_and(from_inner, j == 0))(row_copy(j, third, rows).wait_recv)

        update(j, low2, w2, d2, put, before_diagonal, after_upper, wait_piece)
        return carry

    @pl.when(has_next)
    def _():
        to_next.wait_send()

    @pl.when(has_prev)
    def _():
        to_prev.wait_send()

    @pl.when(inner)
    def _():
        raw = blk.at[:, pl.ds(reach, reach + 1)]
        remote(raw, h1, sem.at[SEND_RAW], recv1.at[0], nxt).wait_send()

    lax.fori_loop(0, rows, second_sweep, 0)

    @pl.when(inner)
    def _():
        part = w2.at[pl.ds(reach, rows), most]
        remote(part, part, sem.at[SEND_ROWS], recv2.at[0], nxt).wait_send()

    def sent_edge():
        for t, w in enumerate((w2, w1)):
            part = w.at[pl.ds(reach, rows)]
            remote(part, part, sem.at[SEND_RAW if t else SEND_ROWS], recv2.at[0], nxt).wait_send()

    only(edge, sent_edge)

    def helped():
        remote(aside, aside, sem.at[SEND_ASIDE], recv2.at[0], nxt).wait_send()

    only(first, helped)

    @pl.when(hands_early)
    def _():
        early_on().wait_send()
    for way, duty in enumerate((by_last, by_first)):
        def passed():
            part = relay.at[:, :, pl.ds(0, ways[way].size)]
            remote(part, part, sem.at[RELAYED], recv2.at[0], nxt).wait_send()

        only(duty, passed)


def per_device(blocks, diag_shift, offsets):
    rows, band, size, _ = blocks.shape
    reach = (band - 1) // 2
    assert rows == reach == 4
    slabs, groups = lax.axis_size("slab"), lax.axis_size("grp")
    shift = diag_shift.reshape(rows, 1, size)
    block = (size, size)
    packed = size // 2 + TILE
    tall = (reach + rows, packed + reach * size, size)
    dma = pltpu.SemaphoreType.DMA
    return pl.pallas_call(
        functools.partial(kernel, slabs, groups, reach),
        out_shape=pltpu.VMEM(blocks.shape, BF16),
        in_specs=[pl.BlockSpec(memory_space=pltpu.HBM)] * 3,
        out_specs=pl.BlockSpec(memory_space=pltpu.VMEM),
        scratch_shapes=[
            pltpu.VMEM(blocks.shape, BF16),
            pltpu.VMEM((2, rows, packed + 2 * size, size), BF16),
            pltpu.VMEM((groups // SPAN - 1,) + block, BF16),
            pltpu.VMEM((EARLY,) + block, BF16),
            pltpu.SMEM((2, rows), jnp.int32),
            pltpu.VMEM((rows, 1, size), F32),
            pltpu.VMEM((AUX, size), F32),
            pltpu.VMEM((SENT, size), F32),
            pltpu.VMEM((SENT, size), F32),
            pltpu.VMEM((3 * rows, 1, size), F32),
            pltpu.VMEM(blocks.shape, BF16),
            pltpu.VMEM(tall, BF16),
            pltpu.VMEM(tall, BF16),
            pltpu.VMEM((reach + rows,) + block, BF16),
            pltpu.VMEM((reach + rows,) + block, BF16),
            pltpu.VMEM((rows, reach) + block, BF16),
            pltpu.VMEM((rows, reach + 1) + block, BF16),
            pltpu.VMEM((reach - 1,) + block, F32),
            dma((7,)), dma((2,)), dma((rows,)), dma((rows + 1,)), dma((2, rows)), dma((1,)),
            pltpu.SemaphoreType.REGULAR((3,)),
        ],
        compiler_params=pltpu.CompilerParams(collective_id=0, has_side_effects=True, vmem_limit_bytes=57 << 20),
    )(blocks, shift, offsets.T)


def solution(mesh):
    return jax.shard_map(
        per_device,
        mesh=mesh,
        in_specs=(
            P(("slab", "grp"), None, None, None),
            P(("slab", "grp")),
            P(("slab", "grp"), None),
        ),
        out_specs=P(("slab", "grp"), None, None, None),
        check_vma=False,
    )
```
